32 devices in a mesh: cohort: 2 (over x), tile: 16 (over z, y, core).
Axes of the slice: x: 2, y: 2, z: 4, core: 2. Of those that a mesh axis runs over, the one named last changes fastest.
Arguments:
- dosage: bfloat16 [512, 8192], P(('cohort', 'tile')), parts along dimension 0, may hold values from 0 to 2
- covars: float32 [512, 16], P(('cohort', 'tile')), parts along dimension 0, may hold values from -12 to 12, as said below
- phenotypes: float32 [512, 1792], P(('cohort', 'tile')), parts along dimension 0, may hold values from -100 to 100
Outputs:
- mean_chi: float32 [3584], P(('cohort', 'tile')), parts along dimension 0
- hit_rate: float32 [3584], P(('cohort', 'tile')), parts along dimension 0
The draws below stay inside these ranges and needn't reach their ends.
There are 2 independent parts, one for each index of `cohort`. The reference program is written for one: setup_inputs(seed, part) draws one part's arguments, and reference() takes and returns one part's arrays. A program takes and returns all parts, laid end to end along the dimension named above; each array names one. Nothing has to cross between parts.
Inputs may be any that keep to these rules, and one draw needn't show every extreme that they name: `covars`: each covariate column has its own mean and spread.
All inputs are finite; a program needn't handle non-finite values.
Results may differ from the reference program's by a relative error of at most 0.003.
Values may be sent and summed in bfloat16 or wider, within the bound.
A program may use at most 64 MiB of HBM per device.

```python
import math
import jax
import jax.numpy as jnp
from jax import lax

VARIANTS = 8192
COVS = 16
SAMPLES = 256
GENES = 1792


def ancestry_score(key):
    label = (jax.random.uniform(jax.random.fold_in(key, 14), (SAMPLES,), jnp.float32) < 0.4).astype(jnp.float32)
    blur = jnp.clip(jax.random.normal(jax.random.fold_in(key, 15), (SAMPLES,), jnp.float32), -4.0, 4.0)
    return label + 0.15 * blur


def covar_table(key):
    base = jnp.clip(jax.random.normal(jax.random.fold_in(key, 11), (SAMPLES, COVS), jnp.float32), -5.0, 5.0)
    score = 2.0 * ancestry_score(key) - 1.0
    base = jnp.concatenate([score[:, None], base[:, 1:]], axis=1)
    means = jax.random.uniform(jax.random.fold_in(key, 12), (COVS,), jnp.float32, -2.0, 2.0)
    spread = jnp.exp(jax.random.uniform(jax.random.fold_in(key, 13), (COVS,), jnp.float32, math.log(0.5), math.log(2.0)))
    return base * spread[None, :] + means[None, :]


def draw_covars(key, part):
    return covar_table(key)


def draw_dosage(key, part):
    score = ancestry_score(key)
    base_freq = jax.random.uniform(jax.random.fold_in(key, 31), (VARIANTS,), jnp.float32, 0.05, 0.95)
    shift = jax.random.uniform(jax.random.fold_in(key, 32), (VARIANTS,), jnp.float32, -0.4, 0.4)
    freq = jnp.clip(base_freq[None, :] + shift[None, :] * (score[:, None] - 0.5), 0.02, 0.98)
    first = (jax.random.uniform(jax.random.fold_in(key, 33), (SAMPLES, VARIANTS), jnp.float32) < freq).astype(jnp.float32)
    second = (jax.random.uniform(jax.random.fold_in(key, 34), (SAMPLES, VARIANTS), jnp.float32) < freq).astype(jnp.float32)
    blur = 0.2 * jnp.clip(jax.random.normal(jax.random.fold_in(key, 35), (SAMPLES, VARIANTS), jnp.float32), -3.0, 3.0)
    return jnp.clip(first + second + blur, 0.0, 2.0).astype(jnp.bfloat16)


def draw_phenotypes(key, part):
    table = covar_table(key)
    effect = jnp.clip(jax.random.normal(jax.random.fold_in(key, 21), (COVS, GENES), jnp.float32), -4.0, 4.0)
    spread = jnp.exp(jax.random.uniform(jax.random.fold_in(key, 22), (GENES,), jnp.float32, math.log(0.5), math.log(2.0)))
    noise = jnp.clip(jax.random.normal(jax.random.fold_in(key, 23), (SAMPLES, GENES), jnp.float32), -8.0, 8.0) * spread[None, :]
    signal = jnp.dot(table, effect, precision=lax.Precision.HIGHEST)
    return jnp.clip(signal + noise, -100.0, 100.0)


def setup_inputs(seed: int = 0, part: int = 0) -> dict:
    streams_of = jax.random.split(jax.random.key(seed), 4)
    own_keys = jax.random.split(jax.random.fold_in(streams_of[3], part), 4)
    dosage = draw_dosage(jax.random.fold_in(jax.random.fold_in(streams_of[3], part), 71), part)
    covars = draw_covars(jax.random.fold_in(jax.random.fold_in(streams_of[3], part), 71), part)
    phenotypes = draw_phenotypes(jax.random.fold_in(jax.random.fold_in(streams_of[3], part), 71), part)
    return dict(dosage=dosage, covars=covars, phenotypes=phenotypes)


def reference(dosage, covars, phenotypes):
    highest = lax.Precision.HIGHEST
    dose_real = dosage.astype(jnp.float32)
    samples = dose_real.shape[0]
    variants = dose_real.shape[1]
    gram = jnp.dot(covars.T.astype(jnp.float32), covars.astype(jnp.float32), precision=highest, preferred_element_type=jnp.float32)
    cov_dose = jnp.dot(covars.T.astype(jnp.float32), dose_real.astype(jnp.float32), precision=highest, preferred_element_type=jnp.float32)
    cov_pheno = jnp.dot(covars.T.astype(jnp.float32), phenotypes.astype(jnp.float32), precision=highest, preferred_element_type=jnp.float32)
    factor = jnp.linalg.cholesky(gram)
    betas = jax.scipy.linalg.cho_solve((factor, True), jnp.concatenate([cov_dose, cov_pheno], axis=1))
    beta_dose = betas[:, :variants]
    beta_pheno = betas[:, variants:]
    dose_resid = dose_real - jnp.dot(covars.astype(jnp.float32), beta_dose.astype(jnp.float32), precision=highest, preferred_element_type=jnp.float32)
    pheno_resid = phenotypes - jnp.dot(covars.astype(jnp.float32), beta_pheno.astype(jnp.float32), precision=highest, preferred_element_type=jnp.float32)
    dose_sumsq = lax.optimization_barrier(jnp.sum(dose_resid * dose_resid, axis=0))
    pheno_sumsq = lax.optimization_barrier(jnp.sum(pheno_resid * pheno_resid, axis=0))
    dose_bf = dose_resid.astype(jnp.bfloat16)
    pheno_bf = pheno_resid.astype(jnp.bfloat16)
    cross = lax.dot_general(pheno_bf.astype(jnp.float32), dose_bf.astype(jnp.float32), (((0,), (0,)), ((), ())), preferred_element_type=jnp.float32)
    dose_var = dose_sumsq / samples + 0.1
    pheno_var = pheno_sumsq / samples + 0.1
    zscore = cross / (jnp.sqrt(jnp.float32(samples)) * jnp.sqrt(pheno_var[:, None] * dose_var[None, :]))
    chi_square = zscore * zscore
    mean_chi = lax.optimization_barrier(jnp.mean(chi_square, axis=1))
    hit_rate = 20.0 / variants * lax.optimization_barrier(jnp.sum(jax.nn.sigmoid(2.0 * (chi_square - 4.0)), axis=1))
    return (mean_chi, hit_rate)
```

```python
import functools

import jax
import jax.numpy as jnp
from jax import lax
from jax.experimental import pallas as pl
from jax.experimental.pallas import tpu as pltpu
from jax.sharding import PartitionSpec as P

LANES = 128
CHUNK = 256
HIGH = lax.Precision.HIGHEST
F32 = jnp.float32
BF16 = jnp.bfloat16


def dot(a, b, ca, cb, precision=None):
    return lax.dot_general(
        a, b, (((ca,), (cb,)), ((), ())), precision=precision, preferred_element_type=F32
    )


def split(a, parts):
    out = []
    for _ in range(parts):
        term = a.astype(BF16)
        out.append(term)
        a = a - term.astype(F32)
    return out


def inverse_factor(gram):
    size = gram.shape[0]
    wide = 2 * size
    row_id = lax.broadcasted_iota(jnp.int32, (size, wide), 0)
    eye = (
        lax.broadcasted_iota(jnp.int32, (size, size), 0)
        == lax.broadcasted_iota(jnp.int32, (size, size), 1)
    ).astype(F32)
    work = jnp.concatenate([gram, eye], axis=1)
    for k in range(0, size, 2):
        one = jnp.broadcast_to(work[:, k : k + 1], (size, wide))
        two = jnp.broadcast_to(work[:, k + 1 : k + 2], (size, wide))
        first = lax.rsqrt(one[k : k + 1, :])
        below = two[k : k + 1, :] * first
        second = lax.rsqrt(two[k + 1 : k + 2, :] - below * below)
        top = work[k : k + 1, :] * first
        low = (work[k + 1 : k + 2, :] - below * top) * second
        left = one * first
        right = (two - left * below) * second
        rest = work - left * top - right * low
        work = jnp.where(
            row_id > k + 1, rest, jnp.where(row_id == k, top, jnp.where(row_id == k + 1, low, work))
        )
    return work[:, size:]


def kernel(
    n, zs, ys, cs, own, group,
    dose_in, cov_in, pheno_in, out_ref,
    dose_ref, pheno_ref, load_sem, cov_all, raw, dose_all, pt, acc, part, landed,
    cov_send, cov_recv, b_send, b_recv, zr_send, zl_send, z_recv, c_send, c_recv,
    d_send, dy_send, d_recv, pass_send, p_recv, part_send, part_recv,
):
    me = lax.axis_index("tile")
    rows, variants = dose_in.shape
    covs = cov_in.shape[1]
    samples = rows * n
    gh = raw.shape[-1]
    width = dose_all.shape[-1]
    peers = n // ys
    c = lax.rem(me, cs)
    y = lax.rem(me // cs, ys)
    z = me // (cs * ys)
    oc = lax.rem(c + 1, cs)
    oy = lax.rem(y + 1, ys)
    place = z * cs + c

    def index(zi, yi, ci):
        return (zi * ys + yi) * cs + ci

    def remote(src, dst, ssem, rsem, dev):
        return pltpu.make_async_remote_copy(
            src_ref=src, dst_ref=dst, send_sem=ssem, recv_sem=rsem,
            device_id={"tile": dev}, device_id_type=pl.DeviceIdType.MESH,
        )

    def lane_slice(start, size):
        return pl.ds(pl.multiple_of(start, LANES), size)

    def peer(k):
        return lax.rem(me + k, n)

    loads = [
        pltpu.make_async_copy(cov_in, cov_all.at[z, c, y], load_sem.at[0]),
        pltpu.make_async_copy(
            pheno_in.at[:, lane_slice(y * gh, gh)], raw.at[z, c, y], load_sem.at[1]
        ),
        pltpu.make_async_copy(
            pheno_in.at[:, lane_slice(oy * gh, gh)], pheno_ref, load_sem.at[2]
        ),
        pltpu.make_async_copy(dose_in, dose_ref, load_sem.at[3]),
        pltpu.make_async_copy(
            dose_in.at[:, lane_slice(place * width, width)], dose_all.at[z, c, y], load_sem.at[4]
        ),
    ]
    for load in loads:
        load.start()
    barrier = pltpu.get_barrier_semaphore()
    for k in range(1, n):
        pl.semaphore_signal(
            barrier, inc=1, device_id={"tile": peer(k)}, device_id_type=pl.DeviceIdType.MESH
        )
    for load in loads:
        load.wait()
    pl.semaphore_wait(barrier, n - 1)

    def cov_copy(k):
        own_cov = cov_all.at[z, c, y]
        return remote(own_cov, own_cov, cov_send.at[k], cov_recv.at[k], peer(k))

    def cov_wait(k):
        src = lax.rem(me + n - k, n)
        slot = cov_all.at[src // (cs * ys), lax.rem(src, cs), lax.rem(src // cs, ys)]
        return remote(slot, slot, cov_send.at[k], cov_recv.at[k], src)

    for k in range(1, n):
        cov_copy(k).start()

    def across():
        return remote(pheno_ref, raw.at[z, c, y], b_send, b_recv, index(z, oy, c))

    def slot_of(p, d):
        return raw.at[p, c, lax.rem(y + d, ys)]

    def to_right(p, d):
        slot = slot_of(p, d)
        return remote(slot, slot, zr_send.at[p, d], z_recv.at[p, d], index(z + 1, y, c))

    def to_left(p, d):
        slot = slot_of(p, d)
        return remote(slot, slot, zl_send.at[p, d], z_recv.at[p, d], index(z - 1, y, c))

    def to_core(p, d):
        slot = slot_of(p, d)
        return remote(slot, slot, c_send.at[p, d], c_recv.at[p], index(z, y, oc))

    def from_core(p):
        slot = raw.at[p, oc]
        return remote(slot, slot, c_send.at[p, 0], c_recv.at[p], index(z, y, oc))

    def spread(d):
        @pl.when(z + 1 < zs)
        def _():
            to_right(z, d).start()

        @pl.when(z > 0)
        def _():
            to_left(z, d).start()

        if cs > 1:
            to_core(z, d).start()

    def dose_copy(p, ci):
        return remote(
            dose_ref.at[:, lane_slice((p * cs + ci) * width, width)], dose_all.at[z, c, y],
            d_send.at[p, ci], d_recv.at[z], index(p, y, ci),
        )

    def dose_across(ci):
        return remote(
            dose_ref.at[:, lane_slice((z * cs + ci) * width, width)], dose_all.at[z, c, y],
            dy_send.at[ci], p_recv.at[z], index(z, oy, ci),
        )

    def dose_pass(p):
        slot = dose_all.at[p, :, y]
        return remote(slot, slot, pass_send.at[p], p_recv.at[p], index(z, oy, c))

    def dose_wait(p):
        slot = dose_all.at[p, :, y]
        return remote(slot, slot, pass_send.at[p], d_recv.at[p], me)

    def across_wait(p):
        slot = dose_all.at[p, :, oy]
        return remote(slot, slot, pass_send.at[p], p_recv.at[p], me)

    def each_side(k, body):
        @pl.when(z >= k)
        def _():
            body(z - k)

        @pl.when(z + k < zs)
        def _():
            body(z + k)

    def send_doses(p):
        for ci in range(cs):
            dose_copy(p, ci).start()

    if ys > 1:
        across().start()
    spread(0)
    if cs > 1:
        dose_copy(z, oc).start()
    if ys > 1:
        for ci in range(cs):
            dose_across(ci).start()
    each_side(1, send_doses)
    if ys > 1:
        remote(pheno_ref, raw.at[z, c, oy], b_send, b_recv, index(z, oy, c)).wait_recv()
        spread(1)
    for k in range(2, zs):
        each_side(k, send_doses)

    def relay(k):
        for d in range(ys):
            @pl.when(z >= k)
            def _():
                p = z - k
                to_right(p, d).wait_recv()

                @pl.when(z + 1 < zs)
                def _():
                    to_right(p, d).start()

                if cs > 1:
                    to_core(p, d).start()

            @pl.when(z + k < zs)
            def _():
                p = z + k
                to_left(p, d).wait_recv()

                @pl.when(z > 0)
                def _():
                    to_left(p, d).start()

                if cs > 1:
                    to_core(p, d).start()

    def hand_on(p):
        dose_wait(p).wait_recv()
        if ys > 1:
            dose_pass(p).start()

    for k in range(1, zs):
        relay(k)
        each_side(k, hand_on)
    if cs > 1:
        slot = dose_all.at[z, oc, y]
        remote(slot, slot, d_send.at[z, oc], d_recv.at[z], me).wait_recv()

    for k in range(1, n):
        cov_wait(k).wait_recv()
    cov = cov_all[...].reshape(samples, covs)
    covt = cov.T
    factor = inverse_factor(dot(covt, cov, 1, 0, HIGH))
    basist = dot(factor, covt, 1, 0, HIGH)
    eye = (
        lax.broadcasted_iota(jnp.int32, (covs, covs), 0)
        == lax.broadcasted_iota(jnp.int32, (covs, covs), 1)
    ).astype(F32)
    fix = 1.5 * eye - 0.5 * dot(basist, basist, 1, 1, HIGH)
    basist = dot(fix, basist, 1, 0, HIGH)
    bt_hi, bt_mid, bt_low = [t.astype(F32) for t in split(basist, 3)]
    bt = jnp.concatenate([bt_hi, bt_mid, bt_low], axis=0).astype(BF16)
    b_hi, b_mid, b_low = [t.astype(F32) for t in split(basist.T, 3)]
    basis = jnp.concatenate([b_hi, b_hi, b_hi, b_mid, b_mid, b_low], axis=1).astype(BF16)

    if cs > 1:
        for p in range(zs):
            from_core(p).wait_recv()

    def residual(at):
        cols = lane_slice(at, LANES)
        pheno = raw[:, :, :, :, cols].reshape(samples, LANES)
        hi, mid, low = split(pheno, 3)
        with_hi = dot(bt, hi, 1, 0)
        with_mid = dot(bt[0 : 2 * covs], mid, 1, 0)
        coef = (
            with_hi[0:covs]
            + (with_hi[covs : 2 * covs] + with_mid[0:covs])
            + (with_hi[2 * covs :] + with_mid[covs:] + dot(bt[0:covs], low, 1, 0))
        )
        one, two, three = [t.astype(F32) for t in split(coef, 3)]
        stack = jnp.concatenate([one, two, three, one, two, one], axis=0).astype(BF16)
        resid = pheno - dot(basis, stack, 1, 0)
        var = jnp.sum(resid * resid, axis=0, keepdims=True) / samples + 0.1
        resid = (resid * lax.rsqrt(var)).T
        hi, low = split(resid, 2)
        genes_at = pl.ds(pl.multiple_of(at, LANES), LANES)
        pt[genes_at, 0:samples] = hi
        pt[genes_at, samples:] = low

    @pl.loop(0, gh // (group * LANES))
    def _(b):
        for g in range(group):
            residual((b * group + g) * LANES)

    if ys > 1:
        for p in range(zs):
            across_wait(p).wait_recv()
    acc[...] = jnp.zeros_like(acc)

    @pl.loop(0, width // CHUNK)
    def _(j):
        dose = dose_all[:, :, :, :, lane_slice(j * CHUNK, CHUNK)].reshape(samples, CHUNK)
        real = dose.astype(F32)
        coef = dot(bt, dose, 1, 0)
        coef = coef[0:covs] + (coef[covs : 2 * covs] + coef[2 * covs :])
        sumsq = jnp.sum(real * real, axis=0, keepdims=True) - jnp.sum(
            coef * coef, axis=0, keepdims=True
        )
        scale = 1.0 / (sumsq + 0.1 * samples)
        twice = jnp.concatenate([dose, dose], axis=0)

        @pl.loop(0, gh // (group * LANES))
        def _(b):
            for g in range(group):
                at = pl.ds(pl.multiple_of((b * group + g) * LANES, LANES), LANES)
                cross = dot(pt[at, :], twice, 1, 0)
                chi = cross * cross * scale
                hit = 1.0 + jnp.tanh(chi - 4.0)
                acc[0, at, :] += sum(chi[:, i : i + LANES] for i in range(0, CHUNK, LANES))
                acc[1, at, :] += sum(hit[:, i : i + LANES] for i in range(0, CHUNK, LANES))

    line = lax.broadcasted_iota(jnp.int32, (8, 4 * LANES), 0)
    lane = lax.broadcasted_iota(jnp.int32, (8, 4 * LANES), 1)
    pick = (lane // (2 * LANES) == line).astype(F32).astype(BF16)

    def part_copy(j):
        return remote(
            part.at[j], landed.at[place], part_send.at[j], part_recv.at[place], y * peers + j
        )

    @pl.loop(0, peers)
    def _(j):
        at = pl.ds(pl.multiple_of(j * own, 8), own)
        terms = split(acc[0, at, :], 2) + split(acc[1, at, :], 2)
        sums = dot(pick, jnp.concatenate(terms, axis=1), 1, 1)
        part[j, :, pl.ds(0, own)] = sums[0:2, :]

        @pl.when(y * peers + j != me)
        def _():
            part_copy(j).start()

    @pl.when(me // peers == y)
    def _():
        landed[place] = part[lax.rem(me, peers)]

    for k in range(1, n):
        cov_copy(k).wait_send()
    if ys > 1:
        across().wait_send()
        for ci in range(cs):
            dose_across(ci).wait_send()
    if cs > 1:
        dose_copy(z, oc).wait_send()
        for p in range(zs):
            for d in range(ys):
                to_core(p, d).wait_send()
    for k in range(zs):
        for d in range(ys):
            @pl.when((z >= k) & (z + 1 < zs))
            def _():
                to_right(z - k, d).wait_send()

            @pl.when((z + k < zs) & (z > 0))
            def _():
                to_left(z + k, d).wait_send()

    def drained(p):
        for ci in range(cs):
            dose_copy(p, ci).wait_send()
        if ys > 1:
            dose_pass(p).wait_send()

    for k in range(1, zs):
        each_side(k, drained)
    for j in range(peers):
        @pl.when(y * peers + j != me)
        def _():
            part_copy(j).wait_send()

    for p in range(peers):
        src = index(p // cs, me // peers, p % cs)

        @pl.when(src != me)
        def _():
            remote(part.at[0], landed.at[p], part_send.at[0], part_recv.at[p], src).wait_recv()

    total = jnp.sum(landed[...], axis=0)
    kind = lax.broadcasted_iota(jnp.int32, total.shape, 0)
    out_ref[...] = jnp.where(kind == 0, total / variants, 10.0 / variants * total)


def local(dosage, covars, phenotypes):
    n = lax.axis_size("tile")
    rows, variants = dosage.shape
    genes = phenotypes.shape[1]
    covs = covars.shape[1]
    samples = rows * n
    cs = 2 if n % 2 == 0 else 1
    ys = 2 if n % (2 * cs) == 0 else 1
    zs = n // (cs * ys)
    peers = zs * cs
    gh = genes // ys
    own = genes // n
    width = variants // peers
    group = max(g for g in range(1, 8) if gh % (g * LANES) == 0)
    dma = pltpu.SemaphoreType.DMA
    out = pl.pallas_call(
        functools.partial(kernel, n, zs, ys, cs, own, group),
        out_shape=jax.ShapeDtypeStruct((2, LANES), F32),
        in_specs=[pl.BlockSpec(memory_space=pl.ANY)] * 3,
        out_specs=pl.BlockSpec(memory_space=pltpu.VMEM),
        scratch_shapes=[
            pltpu.VMEM((rows, variants), BF16),
            pltpu.VMEM((rows, gh), F32),
            dma((5,)),
            pltpu.VMEM((zs, cs, ys, rows, covs), F32),
            pltpu.VMEM((zs, cs, ys, rows, gh), F32),
            pltpu.VMEM((zs, cs, ys, rows, width), BF16),
            pltpu.VMEM((gh, 2 * samples), BF16),
            pltpu.VMEM((2, gh, LANES), F32),
            pltpu.VMEM((peers, 2, LANES), F32),
            pltpu.VMEM((peers, 2, LANES), F32),
            dma((n,)), dma((n,)), dma, dma,
            dma((zs, ys)), dma((zs, ys)), dma((zs, ys)), dma((zs, ys)), dma((zs,)),
            dma((zs, cs)), dma((cs,)), dma((zs,)), dma((zs,)), dma((zs,)),
            dma((peers,)), dma((peers,)),
        ],
        compiler_params=pltpu.CompilerParams(collective_id=0, has_side_effects=True),
    )(dosage, covars, phenotypes)
    return out[0, :own], out[1, :own]


def solution(mesh):
    spec = P(("cohort", "tile"), None)
    return jax.shard_map(
        local,
        mesh=mesh,
        in_specs=(spec, spec, spec),
        out_specs=(P(("cohort", "tile")), P(("cohort", "tile"))),
        check_vma=False,
    )
```

```python
import functools

import jax
import jax.numpy as jnp
from jax import lax
from jax.experimental import pallas as pl
from jax.experimental.pallas import tpu as pltpu
from jax.sharding import PartitionSpec as P

LANES = 128
CHUNK = 256
HIGH = lax.Precision.HIGHEST
F32 = jnp.float32
BF16 = jnp.bfloat16


def dot(a, b, ca, cb, precision=None):
    return lax.dot_general(
        a, b, (((ca,), (cb,)), ((), ())), precision=precision, preferred_element_type=F32
    )


def split(a, parts):
    out = []
    for _ in range(parts):
        term = a.astype(BF16)
        out.append(term)
        a = a - term.astype(F32)
    return out


def begin(copy):
    copy.start()


def sent(copy):
    copy.wait_send()


def inverse_factor(gram):
    size = gram.shape[0]
    wide = 2 * size
    row_id = lax.broadcasted_iota(jnp.int32, (size, wide), 0)
    eye = (
        lax.broadcasted_iota(jnp.int32, (size, size), 0)
        == lax.broadcasted_iota(jnp.int32, (size, size), 1)
    ).astype(F32)
    work = jnp.concatenate([gram, eye], axis=1)
    for k in range(0, size, 2):
        one = jnp.broadcast_to(work[:, k : k + 1], (size, wide))
        two = jnp.broadcast_to(work[:, k + 1 : k + 2], (size, wide))
        first = lax.rsqrt(one[k : k + 1, :])
        below = two[k : k + 1, :] * first
        second = lax.rsqrt(two[k + 1 : k + 2, :] - below * below)
        top = work[k : k + 1, :] * first
        low = (work[k + 1 : k + 2, :] - below * top) * second
        left = one * first
        right = (two - left * below) * second
        rest = work - left * top - right * low
        work = jnp.where(
            row_id > k + 1, rest, jnp.where(row_id == k, top, jnp.where(row_id == k + 1, low, work))
        )
    return work[:, size:]


def scan(
    c, y, z, oc, cs, ys, zs, n, owners, me, place, own, group, halves, hw, samples, covs,
    blocks, cut, cov_all, raw, dose_all, dres, vscale, pt, acc, part, landed, hand_on,
    each_side, cov_wait, pheno_wait, pheno_wait_own, resid_to, resid_pass, resid_wait,
    blocks_here, blocks_over, across_wait, d_recv, remote, part_copy, lane_slice,
):
    far = range(2, zs)
    hand_on(0, [1])

    for k in range(1, n):
        cov_wait(k).wait_recv()
    tiles = cov_all[...].reshape(n, 8, LANES)
    cov = jnp.concatenate(
        [tiles[:, :, i * covs : (i + 1) * covs] for i in range(samples // n // 8)], axis=1
    ).reshape(samples, covs)
    covt = cov.T
    factor = inverse_factor(dot(covt, cov, 1, 0, HIGH))
    basist = dot(factor, covt, 1, 0, HIGH)
    eye = (
        lax.broadcasted_iota(jnp.int32, (covs, covs), 0)
        == lax.broadcasted_iota(jnp.int32, (covs, covs), 1)
    ).astype(F32)
    fix = 1.5 * eye - 0.5 * dot(basist, basist, 1, 1, HIGH)
    basist = dot(fix, basist, 1, 0, HIGH)
    bt_hi, bt_mid, bt_low = [t.astype(F32) for t in split(basist, 3)]
    bt = jnp.concatenate([bt_hi, bt_mid, bt_low], axis=0).astype(BF16)
    b_hi, b_mid, b_low = [t.astype(F32) for t in split(basist.T, 3)]
    basis = jnp.concatenate([b_hi, b_hi, b_hi, b_mid, b_mid, b_low], axis=1).astype(BF16)

    def fitted(coef):
        one, two, three = [t.astype(F32) for t in split(coef, 3)]
        stack = jnp.concatenate([one, two, three, one, two, one], axis=0).astype(BF16)
        return dot(basis, stack, 1, 0)

    def dose_residual(h, j):
        cols = lane_slice(j * CHUNK, CHUNK)
        dose = dose_all[h, :, :, :, :, cols].reshape(samples, CHUNK)
        coef = dot(bt, dose, 1, 0)
        coef = coef[0:covs] + (coef[covs : 2 * covs] + coef[2 * covs :])
        resid = dose.astype(F32) - fitted(coef)
        dres[h, :, cols] = resid.astype(BF16)
        sumsq = jnp.sum(resid * resid, axis=0, keepdims=True)
        vscale[h, :, cols] = 1.0 / (sumsq + 0.1 * samples)

    def dose_residuals(h):
        if cs > 1:
            slot = dose_all.at[h, z, oc, y]
            remote(slot, slot, d_recv.at[h, z], d_recv.at[h, z], me).wait_recv()
        if ys > 1:
            for p in range(zs):
                across_wait(h, p).wait_recv()
        for j in range(hw // CHUNK):
            dose_residual(h, j)

    def arrived(p):
        for d in range(ys):
            pheno_wait(p, d)

    def residual(b, to):
        at = b * LANES
        pheno = raw[:, :, :, :, lane_slice(at, LANES)].reshape(samples, LANES)
        hi, mid, low = split(pheno, 3)
        with_hi = dot(bt, hi, 1, 0)
        with_mid = dot(bt[0 : 2 * covs], mid, 1, 0)
        coef = (
            with_hi[0:covs]
            + (with_hi[covs : 2 * covs] + with_mid[0:covs])
            + (with_hi[2 * covs :] + with_mid[covs:] + dot(bt[0:covs], low, 1, 0))
        )
        resid = pheno - fitted(coef)
        var = jnp.sum(resid * resid, axis=0, keepdims=True) / samples + 0.1
        pt[lane_slice(to * LANES, LANES), :] = (resid * lax.rsqrt(var)).astype(BF16).T

    def residuals():
        for i in range(cut):
            b = place * cut + i
            residual(jnp.minimum(b, blocks - 1), jnp.minimum(b, blocks))
        for i in range(cut):
            resid_to(i, begin)

    def pass_residuals():
        def body(b):
            resid_wait(b).wait_recv()
            if cs > 1:
                resid_pass(b).start()

        blocks_here(body)

    def wait_residuals(own_plane):
        if cs > 1:
            blocks_over(lambda b: resid_pass(b).wait_recv(), own_plane)

    mine = cs * cut
    soon = blocks - (blocks - 1) // mine * mine

    def associate(h, start, stop):
        wide = min(2 * CHUNK, hw)
        count = stop - start
        step = max(g for g in range(1, 8) if count % g == 0)

        @pl.loop(0, hw // wide)
        def _(j):
            cols = lane_slice(j * wide, wide)
            scale = vscale[h, :, cols]

            @pl.loop(0, count // step)
            def _(i):
                for g in range(step):
                    b = lax.rem(place // cs * mine + start + i * step + g, blocks)
                    at = lane_slice(b * LANES, LANES)
                    cross = dot(pt[at, :], dres[h, :, cols], 1, 0)
                    chi = cross * cross * scale
                    hit = 1.0 + jnp.tanh(chi - 4.0)
                    acc[0, at, :] += sum(chi[:, i : i + LANES] for i in range(0, wide, LANES))
                    acc[1, at, :] += sum(hit[:, i : i + LANES] for i in range(0, wide, LANES))

    acc[...] = jnp.zeros_like(acc)
    for h in range(1, halves):
        hand_on(h, [1])
    each_side(arrived)
    if cs > 1:
        for d in range(ys):
            pheno_wait_own(d)
    residuals()
    for h in range(halves):
        hand_on(h, far)
    dose_residuals(0)
    wait_residuals(True)
    associate(0, 0, soon)
    pass_residuals()
    for h in range(1, halves):
        dose_residuals(h)
        associate(h, 0, soon)
    wait_residuals(False)
    for h in range(halves):
        associate(h, soon, blocks)

    line = lax.broadcasted_iota(jnp.int32, (8, 4 * LANES), 0)
    lane = lax.broadcasted_iota(jnp.int32, (8, 4 * LANES), 1)
    pick = (lane // (2 * LANES) == line).astype(F32).astype(BF16)

    @pl.loop(0, owners // 8)
    def _(b):
        for i in range(8):
            j = b * 8 + i
            at = pl.ds(pl.multiple_of(j * own, 8), own)
            terms = split(acc[0, at, :], 2) + split(acc[1, at, :], 2)
            sums = dot(pick, jnp.concatenate(terms, axis=1), 1, 1)
            part[j, :, pl.ds(0, own)] = sums[0:2, :]
        for i in range(8):
            j = b * 8 + i

            @pl.when(y * owners + j != me)
            def _():
                part_copy(j).start()

    @pl.when(me // owners == y)
    def _():
        landed[place] = part[lax.rem(me, owners)]


def kernel(
    n, zs, ys, cs, lo, hi, own, group,
    dose_in, cov_in, pheno_in, out_ref,
    dose_ref, cov_ref, pheno_ref, load_sem, cov_all, raw, dose_all, dres, vscale, pt, acc, part, landed,
    cov_send, cov_recv, b_send, b_recv, a_send, a_core, a_recv,
    x_send, xo_send, x_recv, xc_send, xc_recv,
    d_send, dy_send, d_recv, pass_send, p_recv, part_send, part_recv,
):
    me = lax.axis_index("tile")
    rows, variants = dose_in.shape
    covs = cov_in.shape[1]
    samples = rows * n
    gh = raw.shape[-1]
    halves = dose_all.shape[0]
    hw = dose_all.shape[-1]
    width = halves * hw
    nc = hi - lo
    owners = n // ys
    c = lax.rem(me, cs)
    y = lax.rem(me // cs, ys)
    z = me // (cs * ys)
    oc = lax.rem(c + 1, cs)
    oy = lax.rem(y + 1, ys)
    place = (z - lo) * cs + c
    mid = (z >= lo) & (z < hi)
    far = (2 * z) // zs

    def index(zi, yi, ci):
        return (zi * ys + yi) * cs + ci

    def remote(src, dst, ssem, rsem, dev):
        return pltpu.make_async_remote_copy(
            src_ref=src, dst_ref=dst, send_sem=ssem, recv_sem=rsem,
            device_id={"tile": dev}, device_id_type=pl.DeviceIdType.MESH,
        )

    def lane_slice(start, size):
        return pl.ds(pl.multiple_of(start, LANES), size)

    loads = [
        pltpu.make_async_copy(cov_in, cov_ref, load_sem.at[0]),
        pltpu.make_async_copy(
            pheno_in.at[:, lane_slice(oy * gh, gh)], pheno_ref, load_sem.at[2]
        ),
        pltpu.make_async_copy(
            pheno_in.at[:, lane_slice(y * gh, gh)], raw.at[z, c, y], load_sem.at[1]
        ),
        pltpu.make_async_copy(dose_in, dose_ref, load_sem.at[3]),
    ]

    def own_dose(h):
        return pltpu.make_async_copy(
            dose_in.at[:, lane_slice(place * width + h * hw, hw)],
            dose_all.at[h, z, c, y], load_sem.at[4 + h],
        )

    for load in loads:
        load.start()

    @pl.when(mid)
    def _():
        for h in range(halves):
            own_dose(h).start()

    barrier = pltpu.get_barrier_semaphore()

    def greet(dev):
        pl.semaphore_signal(
            barrier, inc=1, device_id={"tile": dev}, device_id_type=pl.DeviceIdType.MESH
        )

    @pl.when(mid)
    def _():
        for k in range(1, n):
            greet(lax.rem(me + k, n))

    if ys > 1:
        @pl.when(jnp.logical_not(mid))
        def _():
            greet(index(z, oy, c))

    for load in loads:
        load.wait()
    packed = [cov_ref[g : g + 8, :] for g in range(0, rows, 8)]
    fill = jnp.zeros((8, LANES - len(packed) * covs), F32)
    cov_all[z, c, y] = jnp.concatenate(packed + [fill], axis=1)

    @pl.when(mid)
    def _():
        for h in range(halves):
            own_dose(h).wait()
        pl.semaphore_wait(barrier, nc * ys * cs - 1)

    @pl.when(jnp.logical_not(mid))
    def _():
        pl.semaphore_wait(barrier, nc * ys * cs + (1 if ys > 1 else 0))

    def plane(i, body):
        p = jnp.where(mid, lo + lax.rem(z - lo + 1 + i + nc, nc), lo + i + far * (nc - 1 - 2 * i))

        @pl.when(p != z)
        def _():
            body(p)

    def planes(body):
        for i in range(nc):
            plane(i, body)

    def cov_copies(act):
        own_cov = cov_all.at[z, c, y]
        for j in range(nc * ys * cs):
            dev = lo * ys * cs + j

            @pl.when(dev != me)
            def _():
                act(remote(own_cov, own_cov, cov_send.at[j], cov_recv.at[me], dev))

    def cov_wait(k):
        src = lax.rem(me + n - k, n)
        slot = cov_all.at[src // (cs * ys), lax.rem(src, cs), lax.rem(src // cs, ys)]
        return remote(slot, slot, cov_send.at[0], cov_recv.at[src], me)

    def across():
        return remote(pheno_ref, raw.at[z, c, y], b_send, b_recv, index(z, oy, c))

    blocks = gh // LANES
    cut = -(-blocks // (nc * cs))

    def first(q):
        return jnp.minimum(q * cut, blocks - cut)

    def raw_slot(p, ci, d, q):
        return raw.at[p, ci, lax.rem(y + d, ys), :, lane_slice(first(q) * LANES, cut * LANES)]

    def pheno_to(d, act):
        def to(p):
            for ci in range(cs):
                slot = raw_slot(z, c, d, (p - lo) * cs + ci)
                act(
                    remote(
                        slot, slot, a_send.at[p - lo, ci, d], a_recv.at[z, d], index(p, y, ci)
                    )
                )

        return to

    def pheno_over(d, act):
        if cs > 1:
            @pl.when(mid)
            def _():
                slot = raw_slot(z, c, d, (z - lo) * cs + oc)
                act(remote(slot, slot, a_core.at[d], a_recv.at[z, d], index(z, y, oc)))

    def pheno_wait(p, d):
        slot = raw_slot(p, pl.ds(0, cs), d, place)
        remote(slot, slot, a_core.at[d], a_recv.at[p, d], me).wait_recv()

    def pheno_wait_own(d):
        slot = raw_slot(z, oc, d, place)
        remote(slot, slot, a_core.at[d], a_recv.at[z, d], me).wait_recv()

    def resid_slot(b):
        return pt.at[pl.ds(pl.multiple_of(b * LANES, LANES), LANES)]

    def resid_to(i, act):
        b = place * cut + i

        @pl.when(b < blocks)
        def _():
            for j in range(1, nc):
                p = lo + lax.rem(z - lo + j, nc)
                act(
                    remote(
                        resid_slot(b), resid_slot(b), x_send.at[i, j], x_recv.at[b], index(p, y, c)
                    )
                )
            if cs > 1:
                act(
                    remote(
                        resid_slot(b), resid_slot(b), xo_send.at[i], xc_recv.at[b], index(z, y, oc)
                    )
                )

    def resid_pass(b):
        return remote(
            resid_slot(b), resid_slot(b), xc_send.at[b], xc_recv.at[b], index(z, y, oc)
        )

    def resid_wait(b):
        return remote(resid_slot(b), resid_slot(b), xc_send.at[b], x_recv.at[b], me)

    def blocks_here(body):
        for b in range(blocks):
            q = b // cut

            @pl.when((c == q % cs) & (z != lo + q // cs))
            def _():
                body(b)

    def blocks_over(body, own_plane):
        for b in range(blocks):
            q = b // cut
            near = z == lo + q // cs

            @pl.when((c != q % cs) & (near if own_plane else jnp.logical_not(near)))
            def _():
                body(b)

    def block(p, ci, h):
        return dose_ref.at[:, lane_slice(((p - lo) * cs + ci) * width + h * hw, hw)]

    def dose_to(h, act):
        def to(p):
            for ci in range(cs):
                act(
                    remote(
                        block(p, ci, h), dose_all.at[h, z, c, y],
                        d_send.at[h, p - lo, ci], d_recv.at[h, z], index(p, y, ci),
                    )
                )

        return to

    def own_copies(h, act):
        @pl.when(mid)
        def _():
            if ys > 1:
                for ci in range(cs):
                    act(
                        remote(
                            block(z, ci, h), dose_all.at[h, z, c, y],
                            dy_send.at[h, ci], p_recv.at[h, z], index(z, oy, ci),
                        )
                    )
            if cs > 1:
                act(
                    remote(
                        block(z, oc, h), dose_all.at[h, z, c, y],
                        d_send.at[h, z - lo, oc], d_recv.at[h, z], index(z, y, oc),
                    )
                )

    def dose_pass(h, p):
        slot = dose_all.at[h, p, :, y]
        return remote(slot, slot, pass_send.at[h, p], p_recv.at[h, p], index(z, oy, c))

    def dose_wait(h, p):
        slot = dose_all.at[h, p, :, y]
        return remote(slot, slot, pass_send.at[h, p], d_recv.at[h, p], me)

    def across_wait(h, p):
        slot = dose_all.at[h, p, :, oy]
        return remote(slot, slot, pass_send.at[h, p], p_recv.at[h, p], me)

    def at_distance(k, body):
        @pl.when(z >= k)
        def _():
            body(z - k)

        @pl.when(z + k < zs)
        def _():
            body(z + k)

    def each_side(body):
        for k in range(1, zs):
            at_distance(k, body)

    def hand_on(h, ks):
        def body(p):
            dose_wait(h, p).wait_recv()
            if ys > 1:
                dose_pass(h, p).start()

        for k in ks:
            at_distance(k, body)

    if ys > 1:
        across().start()
    own_copies(0, begin)
    plane(0, dose_to(0, begin))
    cov_copies(begin)
    for h in range(1, halves):
        own_copies(h, begin)
        plane(0, dose_to(h, begin))
    pheno_over(0, begin)
    for i in range(nc):
        plane(i, pheno_to(0, begin))
    if ys > 1:
        slot = raw.at[z, c, oy]
        remote(slot, slot, b_send, b_recv, me).wait_recv()
        pheno_over(1, begin)
        for i in range(nc):
            plane(i, pheno_to(1, begin))
    for i in range(1, nc):
        for h in range(halves):
            plane(i, dose_to(h, begin))

    def part_copy(j):
        return remote(
            part.at[j], landed.at[place], part_send.at[j], part_recv.at[place], y * owners + j
        )

    @pl.when(mid)
    def _():
        scan(
            c, y, z, oc, cs, ys, zs, n, owners, me, place, own, group, halves, hw, samples,
            covs, blocks, cut, cov_all, raw, dose_all, dres, vscale, pt, acc, part, landed,
            hand_on, each_side, cov_wait, pheno_wait, pheno_wait_own, resid_to,
            resid_pass, resid_wait, blocks_here, blocks_over, across_wait, d_recv, remote, part_copy,
            lane_slice,
        )

    if ys > 1:
        across().wait_send()
    cov_copies(sent)
    for d in range(ys):
        pheno_over(d, sent)
        planes(pheno_to(d, sent))
    for h in range(halves):
        own_copies(h, sent)
        planes(dose_to(h, sent))

    @pl.when(mid)
    def _():
        for i in range(cut):
            resid_to(i, sent)
        if cs > 1:
            blocks_here(lambda b: resid_pass(b).wait_send())
        if ys > 1:
            for h in range(halves):
                each_side(lambda p: dose_pass(h, p).wait_send())

    for p in range(nc * cs):
        src = index(lo + p // cs, me // owners, p % cs)

        @pl.when(src != me)
        def _():
            remote(part.at[0], landed.at[p], part_send.at[0], part_recv.at[p], me).wait_recv()

    total = jnp.sum(landed[...], axis=0)
    kind = lax.broadcasted_iota(jnp.int32, total.shape, 0)
    out_ref[...] = jnp.where(kind == 0, total / variants, 10.0 / variants * total)

    @pl.when(mid)
    def _():
        for j in range(owners):
            @pl.when(y * owners + j != me)
            def _():
                part_copy(j).wait_send()


def local(dosage, covars, phenotypes):
    n = lax.axis_size("tile")
    rows, variants = dosage.shape
    genes = phenotypes.shape[1]
    covs = covars.shape[1]
    samples = rows * n
    cs = 2 if n % 2 == 0 else 1
    ys = 2 if n % (2 * cs) == 0 else 1
    zs = n // (cs * ys)
    lo, hi = zs // 4, zs - zs // 4
    peers = (hi - lo) * cs
    owners = n // ys
    gh = genes // ys
    own = genes // n
    halves = 2
    hw = variants // peers // halves
    blocks = gh // LANES
    group = max(g for g in range(1, 8) if blocks % g == 0)
    dma = pltpu.SemaphoreType.DMA
    out = pl.pallas_call(
        functools.partial(kernel, n, zs, ys, cs, lo, hi, own, group),
        out_shape=pltpu.VMEM((2, LANES), F32),
        in_specs=[pl.BlockSpec(memory_space=pl.ANY)] * 3,
        out_specs=pl.BlockSpec(memory_space=pltpu.VMEM),
        scratch_shapes=[
            pltpu.VMEM((rows, variants), BF16),
            pltpu.VMEM((rows, covs), F32),
            pltpu.VMEM((rows, gh), F32),
            dma((4 + halves,)),
            pltpu.VMEM((zs, cs, ys, 8, LANES), F32),
            pltpu.VMEM((zs, cs, ys, rows, gh), F32),
            pltpu.VMEM((halves, zs, cs, ys, rows, hw), BF16),
            pltpu.VMEM((halves, samples, hw), BF16),
            pltpu.VMEM((halves, 1, hw), F32),
            pltpu.VMEM((gh + LANES, samples), BF16),
            pltpu.VMEM((2, gh, LANES), F32),
            pltpu.VMEM((owners, 2, LANES), F32),
            pltpu.VMEM((peers, 2, LANES), F32),
            dma((n,)), dma((n,)), dma, dma,
            dma((hi - lo, cs, ys)), dma((ys,)), dma((zs, ys)),
            dma((blocks, hi - lo)), dma((blocks,)), dma((blocks,)), dma((blocks,)), dma((blocks,)),
            dma((halves, hi - lo, cs)), dma((halves, cs)), dma((halves, zs)),
            dma((halves, zs)), dma((halves, zs)),
            dma((owners,)), dma((peers,)),
        ],
        compiler_params=pltpu.CompilerParams(collective_id=0, has_side_effects=True),
    )(dosage, covars, phenotypes)
    return out[0, :own], out[1, :own]


def solution(mesh):
    spec = P(("cohort", "tile"), None)
    return jax.shard_map(
        local,
        mesh=mesh,
        in_specs=(spec, spec, spec),
        out_specs=(P(("cohort", "tile")), P(("cohort", "tile"))),
        check_vma=False,
    )
```

```python
import functools

import jax
import jax.numpy as jnp
from jax import lax
from jax.experimental import pallas as pl
from jax.experimental.pallas import tpu as pltpu
from jax.sharding import PartitionSpec as P

LANES = 128
CHUNK = 256
HIGH = lax.Precision.HIGHEST
F32 = jnp.float32
BF16 = jnp.bfloat16


def dot(a, b, ca, cb, precision=None):
    return lax.dot_general(
        a, b, (((ca,), (cb,)), ((), ())), precision=precision, preferred_element_type=F32
    )


def split(a, parts):
    out = []
    for _ in range(parts):
        term = a.astype(BF16)
        out.append(term)
        a = a - term.astype(F32)
    return out


def inverse_factor(gram):
    size = gram.shape[0]
    wide = 2 * size
    row_id = lax.broadcasted_iota(jnp.int32, (size, wide), 0)
    eye = (
        lax.broadcasted_iota(jnp.int32, (size, size), 0)
        == lax.broadcasted_iota(jnp.int32, (size, size), 1)
    ).astype(F32)
    work = jnp.concatenate([gram, eye], axis=1)
    for k in range(0, size, 2):
        one = jnp.broadcast_to(work[:, k : k + 1], (size, wide))
        two = jnp.broadcast_to(work[:, k + 1 : k + 2], (size, wide))
        first = lax.rsqrt(one[k : k + 1, :])
        below = two[k : k + 1, :] * first
        second = lax.rsqrt(two[k + 1 : k + 2, :] - below * below)
        top = work[k : k + 1, :] * first
        low = (work[k + 1 : k + 2, :] - below * top) * second
        left = one * first
        right = (two - left * below) * second
        rest = work - left * top - right * low
        work = jnp.where(
            row_id > k + 1, rest, jnp.where(row_id == k, top, jnp.where(row_id == k + 1, low, work))
        )
    return work[:, size:]


def scan(
    c, y, z, oc, other_row, cs, ys, zs, n, owners, me, place, own, halves, hw, samples, covs,
    blocks, cut, cov_all, raw, dose_all, dres, vscale, pt, acc, part, landed, hand_on, cov_wait,
    pheno_wait, resid_to, resid_pass, resid_wait, blocks_here, blocks_over, across_wait, d_recv,
    remote, send_part, in_group, lane_slice,
):
    far = range(2, zs)
    hand_on(0, [1])

    cov_wait(n - 1)
    tiles = cov_all[...]
    cov = jnp.concatenate(
        [tiles[:, :, i * covs : (i + 1) * covs] for i in range(samples // n // 8)], axis=1
    ).reshape(samples, covs)
    covt = cov.T
    factor = inverse_factor(dot(covt, cov, 1, 0, HIGH))
    basist = dot(factor, covt, 1, 0, HIGH)
    eye = (
        lax.broadcasted_iota(jnp.int32, (covs, covs), 0)
        == lax.broadcasted_iota(jnp.int32, (covs, covs), 1)
    ).astype(F32)
    fix = 1.5 * eye - 0.5 * dot(basist, basist, 1, 1, HIGH)
    basist = dot(fix, basist, 1, 0, HIGH)
    bt_hi, bt_mid, bt_low = [t.astype(F32) for t in split(basist, 3)]
    bt = jnp.concatenate([bt_hi, bt_mid, bt_low], axis=0).astype(BF16)
    b_hi, b_mid, b_low = [t.astype(F32) for t in split(basist.T, 3)]
    basis = jnp.concatenate([b_hi, b_hi, b_hi, b_mid, b_mid, b_low], axis=1).astype(BF16)

    def fitted(coef):
        one, two, three = [t.astype(F32) for t in split(coef, 3)]
        stack = jnp.concatenate([one, two, three, one, two, one], axis=0).astype(BF16)
        return dot(basis, stack, 1, 0)

    def dose_residual(h, j):
        cols = lane_slice(j * CHUNK, CHUNK)
        dose = dose_all[h, :, :, :, cols].reshape(samples, CHUNK)
        coef = dot(bt, dose, 1, 0)
        coef = coef[0:covs] + (coef[covs : 2 * covs] + coef[2 * covs :])
        resid = dose.astype(F32) - fitted(coef)
        dres[h, :, cols] = resid.astype(BF16)
        sumsq = jnp.sum(resid * resid, axis=0, keepdims=True)
        vscale[h, :, cols] = 1.0 / (sumsq + 0.1 * samples)

    def dose_residuals(h):
        if cs > 1:
            slot = dose_all.at[h, other_row, y]
            remote(slot, slot, d_recv.at[h, z], d_recv.at[h, z], me).wait_recv()
        if ys > 1:
            across_wait(h)
        for j in range(hw // CHUNK):
            dose_residual(h, j)

    def residual(b, to):
        at = b * LANES
        pheno = raw[:, :, :, lane_slice(at, LANES)].reshape(samples, LANES)
        hi, mid, low = split(pheno, 3)
        with_hi = dot(bt, hi, 1, 0)
        with_mid = dot(bt[0 : 2 * covs], mid, 1, 0)
        coef = (
            with_hi[0:covs]
            + (with_hi[covs : 2 * covs] + with_mid[0:covs])
            + (with_hi[2 * covs :] + with_mid[covs:] + dot(bt[0:covs], low, 1, 0))
        )
        resid = pheno - fitted(coef)
        var = jnp.sum(resid * resid, axis=0, keepdims=True) / samples + 0.1
        pt[lane_slice(to * LANES, LANES), :] = (resid * lax.rsqrt(var)).astype(BF16).T

    def residuals():
        for i in range(cut):
            b = place * cut + i
            residual(jnp.minimum(b, blocks - 1), jnp.minimum(b, blocks))
        for i in range(cut):
            resid_to(i)

    def pass_residuals():
        def body(b):
            resid_wait(b).wait_recv()
            if cs > 1:
                resid_pass(b).start()

        blocks_here(body)

    def wait_residuals(own_plane):
        if cs > 1:
            blocks_over(lambda b: resid_pass(b).wait_recv(), own_plane)

    mine = cs * cut
    soon = blocks - (blocks - 1) // mine * mine

    def associate(h, start, stop):
        wide = min(2 * CHUNK, hw)
        count = stop - start
        step = max(g for g in range(1, 8) if count % g == 0)

        @pl.loop(0, hw // wide)
        def _(j):
            cols = lane_slice(j * wide, wide)
            scale = vscale[h, :, cols]

            @pl.loop(0, count // step)
            def _(i):
                for g in range(step):
                    b = lax.rem(place // cs * mine + start + i * step + g, blocks)
                    at = lane_slice(b * LANES, LANES)
                    cross = dot(pt[at, :], dres[h, :, cols], 1, 0)
                    chi = cross * cross * scale
                    hit = 1.0 + jnp.tanh(chi - 4.0)
                    acc[0, at, :] += sum(chi[:, i : i + LANES] for i in range(0, wide, LANES))
                    acc[1, at, :] += sum(hit[:, i : i + LANES] for i in range(0, wide, LANES))

    acc[...] = jnp.zeros_like(acc)
    for h in range(1, halves):
        hand_on(h, [1])
    pheno_wait(zs * cs - 1)
    residuals()
    for h in range(halves):
        hand_on(h, far)
    dose_residuals(0)
    wait_residuals(True)
    associate(0, 0, soon)
    pass_residuals()
    for h in range(1, halves):
        dose_residuals(h)
        associate(h, 0, soon)
    wait_residuals(False)
    for h in range(halves):
        associate(h, soon, blocks)

    line = lax.broadcasted_iota(jnp.int32, (8, 4 * LANES), 0)
    lane = lax.broadcasted_iota(jnp.int32, (8, 4 * LANES), 1)
    pick = (lane // (2 * LANES) == line).astype(F32).astype(BF16)

    @pl.loop(0, owners // 8)
    def _(b):
        for i in range(8):
            j = b * 8 + i
            at = pl.ds(pl.multiple_of(j * own, 8), own)
            terms = split(acc[0, at, :], 2) + split(acc[1, at, :], 2)
            sums = dot(pick, jnp.concatenate(terms, axis=1), 1, 1)
            part[j, :, pl.ds(0, own)] = sums[0:2, :]
        for i in range(8):
            j = b * 8 + i

            @pl.when(y * owners + j != me)
            def _():
                send_part(j)

    @pl.when(in_group)
    def _():
        landed[place] = part[lax.rem(me, owners)]


def kernel(
    n, zs, ys, cs, lo, hi, own,
    dose_in, cov_in, pheno_in, out_ref,
    dose_ref, cov_ref, pheno_ref, load_sem, sends, cov_all, raw, dose_all, dres, vscale, pt, acc,
    part, landed, recvs, x_sem, d_recv, p_recv,
):
    me = lax.axis_index("tile")
    rows, variants = dose_in.shape
    covs = cov_in.shape[1]
    samples = rows * n
    gh = raw.shape[-1]
    halves = dose_all.shape[0]
    hw = dose_all.shape[-1]
    width = halves * hw
    nc = hi - lo
    owners = n // ys
    c = lax.rem(me, cs)
    y = lax.rem(me // cs, ys)
    z = me // (cs * ys)
    oc = lax.rem(c + 1, cs)
    oy = lax.rem(y + 1, ys)
    place = (z - lo) * cs + c
    own_row = z * cs + c
    other_row = z * cs + oc
    cov_send, b_send, a_send, d_send, pass_send, part_send, xc_send = [sends.at[i] for i in range(7)]
    cov_recv, b_recv, a_recv, part_recv = [recvs.at[i] for i in range(4)]
    mid = (z >= lo) & (z < hi)
    far = (2 * z) // zs

    def index(zi, yi, ci):
        return (zi * ys + yi) * cs + ci

    def remote(src, dst, ssem, rsem, dev):
        return pltpu.make_async_remote_copy(
            src_ref=src, dst_ref=dst, send_sem=ssem, recv_sem=rsem,
            device_id={"tile": dev}, device_id_type=pl.DeviceIdType.MESH,
        )

    def lane_slice(start, size):
        return pl.ds(pl.multiple_of(start, LANES), size)

    loads = [
        pltpu.make_async_copy(cov_in, cov_ref, load_sem.at[0]),
        pltpu.make_async_copy(
            pheno_in.at[:, lane_slice(oy * gh, gh)], pheno_ref, load_sem.at[2]
        ),
        pltpu.make_async_copy(
            pheno_in.at[:, lane_slice(y * gh, gh)], raw.at[own_row, y], load_sem.at[1]
        ),
        pltpu.make_async_copy(dose_in, dose_ref, load_sem.at[3]),
    ]

    def own_dose(h):
        return pltpu.make_async_copy(
            dose_in.at[:, lane_slice(place * width + h * hw, hw)],
            dose_all.at[h, own_row, y], load_sem.at[4 + h],
        )

    for load in loads:
        load.start()

    @pl.when(mid)
    def _():
        for h in range(halves):
            own_dose(h).start()

    barrier = pltpu.get_barrier_semaphore()

    def greet(dev):
        pl.semaphore_signal(
            barrier, inc=1, device_id={"tile": dev}, device_id_type=pl.DeviceIdType.MESH
        )

    @pl.when(mid)
    def _():
        for k in range(1, n):
            greet(lax.rem(me + k, n))

    if ys > 1:
        @pl.when(jnp.logical_not(mid))
        def _():
            greet(index(z, oy, c))

    for load in loads:
        load.wait()
    packed = [cov_ref[g : g + 8, :] for g in range(0, rows, 8)]
    fill = jnp.zeros((8, LANES - len(packed) * covs), F32)
    cov_all[own_row * ys + y] = jnp.concatenate(packed + [fill], axis=1)

    @pl.when(mid)
    def _():
        for h in range(halves):
            own_dose(h).wait()
        pl.semaphore_wait(barrier, nc * ys * cs - 1)

    @pl.when(jnp.logical_not(mid))
    def _():
        pl.semaphore_wait(barrier, nc * ys * cs + (1 if ys > 1 else 0))

    def plane(i, body):
        p = jnp.where(mid, lo + lax.rem(z - lo + 1 + i + nc, nc), lo + i + far * (nc - 1 - 2 * i))

        @pl.when(p != z)
        def _():
            body(p)

    def planes(body):
        for i in range(nc):
            plane(i, body)

    def cov_copies():
        own_cov = cov_all.at[own_row * ys + y]
        for j in range(nc * ys * cs):
            dev = lo * ys * cs + j

            @pl.when(dev != me)
            def _():
                remote(own_cov, own_cov, cov_send, cov_recv, dev).start()

    def cov_wait(count, send=False):
        slot = cov_all.at[pl.ds(0, count)]
        copy = remote(slot, slot, cov_send, cov_recv, me)
        if send:
            copy.wait_send()
        else:
            copy.wait_recv()

    def across():
        return remote(pheno_ref, raw.at[own_row, y], b_send, b_recv, index(z, oy, c))

    blocks = gh // LANES
    cut = -(-blocks // (nc * cs))

    def first(q):
        return jnp.minimum(q * cut, blocks - cut)

    def raw_slot(d, q):
        lanes = lane_slice(first(q) * LANES, cut * LANES)
        return raw.at[own_row, lax.rem(y + d, ys), :, lanes]

    def pheno_to(d):
        def to(p):
            for ci in range(cs):
                slot = raw_slot(d, (p - lo) * cs + ci)
                remote(slot, slot, a_send, a_recv, index(p, y, ci)).start()

        return to

    def pheno_over(d):
        if cs > 1:
            @pl.when(mid)
            def _():
                slot = raw_slot(d, (z - lo) * cs + oc)
                remote(slot, slot, a_send, a_recv, index(z, y, oc)).start()

    def pheno_wait(count, send=False):
        slot = raw.at[pl.ds(0, count), :, :, pl.ds(0, cut * LANES)]
        copy = remote(slot, slot, a_send, a_recv, me)
        if send:
            copy.wait_send()
        else:
            copy.wait_recv()

    def resid_slot(b):
        return pt.at[pl.ds(pl.multiple_of(b * LANES, LANES), LANES)]

    def resid_to(i):
        b = place * cut + i

        @pl.when(b < blocks)
        def _():
            for j in range(1, nc):
                p = lo + lax.rem(z - lo + j, nc)
                remote(
                    resid_slot(b), resid_slot(b), x_sem.at[0, 0, i], x_sem.at[z - lo, 1, i],
                    index(p, y, c),
                ).start()
            if cs > 1:
                remote(
                    resid_slot(b), resid_slot(b), x_sem.at[0, 0, i], x_sem.at[z - lo, 2, i],
                    index(z, y, oc),
                ).start()

    def resid_sent(i):
        slot = pt.at[pl.ds(0, (nc - 1 + (1 if cs > 1 else 0)) * LANES)]

        @pl.when(place * cut + i < blocks)
        def _():
            remote(slot, slot, x_sem.at[0, 0, i], x_sem.at[0, 1, i], me).wait_send()

    def resid_pass(b):
        source = b // cut // cs
        return remote(
            resid_slot(b), resid_slot(b), xc_send, x_sem.at[source, 2, b % cut], index(z, y, oc)
        )

    def resid_wait(b):
        source = b // cut // cs
        return remote(resid_slot(b), resid_slot(b), xc_send, x_sem.at[source, 1, b % cut], me)

    def blocks_here(body):
        for b in range(blocks):
            q = b // cut

            @pl.when((c == q % cs) & (z != lo + q // cs))
            def _():
                body(b)

    def blocks_over(body, own_plane):
        for b in range(blocks):
            q = b // cut
            near = z == lo + q // cs

            @pl.when((c != q % cs) & (near if own_plane else jnp.logical_not(near)))
            def _():
                body(b)

    def passed_all():
        for at in range(nc):
            for ci in range(cs):
                count = sum(b // cut % cs == ci and b // cut // cs != at for b in range(blocks))
                if count:
                    slot = pt.at[pl.ds(0, count * LANES)]

                    @pl.when((z == lo + at) & (c == ci))
                    def _():
                        remote(slot, slot, xc_send, xc_send, me).wait_send()

    def block(p, ci, h):
        return dose_ref.at[:, lane_slice(((p - lo) * cs + ci) * width + h * hw, hw)]

    def dose_to(h):
        def to(p):
            for ci in range(cs):
                remote(
                    block(p, ci, h), dose_all.at[h, own_row, y], d_send, d_recv.at[h, z],
                    index(p, y, ci),
                ).start()

        return to

    def own_copies(h):
        @pl.when(mid)
        def _():
            if ys > 1:
                for ci in range(cs):
                    remote(
                        block(z, ci, h), dose_all.at[h, own_row, y], d_send, p_recv.at[h],
                        index(z, oy, ci),
                    ).start()
            if cs > 1:
                remote(
                    block(z, oc, h), dose_all.at[h, own_row, y], d_send, d_recv.at[h, z],
                    index(z, y, oc),
                ).start()

    def dose_sent(count):
        slot = dose_all.at[:, pl.ds(0, count), 0]
        remote(slot, slot, d_send, d_recv.at[0, 0], me).wait_send()

    def dose_pass(h, p):
        slot = dose_all.at[h, pl.ds(p * cs, cs), y]
        return remote(slot, slot, pass_send, p_recv.at[h], index(z, oy, c))

    def passes_sent():
        slot = dose_all.at[:, pl.ds(0, (zs - 1) * cs), 0]
        remote(slot, slot, pass_send, p_recv.at[0], me).wait_send()

    def dose_wait(h, p):
        slot = dose_all.at[h, pl.ds(p * cs, cs), y]
        return remote(slot, slot, pass_send, d_recv.at[h, p], me)

    def across_wait(h):
        slot = dose_all.at[h, :, oy]
        remote(slot, slot, pass_send, p_recv.at[h], me).wait_recv()

    def at_distance(k, body):
        @pl.when(z >= k)
        def _():
            body(z - k)

        @pl.when(z + k < zs)
        def _():
            body(z + k)

    def hand_on(h, ks):
        def body(p):
            dose_wait(h, p).wait_recv()
            if ys > 1:
                dose_pass(h, p).start()

        for k in ks:
            at_distance(k, body)

    if ys > 1:
        across().start()
    own_copies(0)
    plane(0, dose_to(0))
    cov_copies()
    for h in range(1, halves):
        own_copies(h)
        plane(0, dose_to(h))
    pheno_over(0)
    for i in range(nc):
        plane(i, pheno_to(0))
    if ys > 1:
        slot = raw.at[own_row, oy]
        remote(slot, slot, b_send, b_recv, me).wait_recv()
        pheno_over(1)
        for i in range(nc):
            plane(i, pheno_to(1))
    for i in range(1, nc):
        for h in range(halves):
            plane(i, dose_to(h))

    in_group = mid & (me // owners == y)

    def send_part(j):
        remote(part.at[j], landed.at[place], part_send, part_recv, y * owners + j).start()

    @pl.when(mid)
    def _():
        scan(
            c, y, z, oc, other_row, cs, ys, zs, n, owners, me, place, own, halves, hw, samples,
            covs, blocks, cut, cov_all, raw, dose_all, dres, vscale, pt, acc, part, landed,
            hand_on, cov_wait, pheno_wait, resid_to, resid_pass, resid_wait, blocks_here,
            blocks_over, across_wait, d_recv, remote, send_part, in_group, lane_slice,
        )

    if ys > 1:
        across().wait_send()

    @pl.when(mid)
    def _():
        cov_wait(nc * ys * cs - 1, send=True)
        pheno_wait((nc - 1) * cs + (1 if cs > 1 else 0), send=True)
        dose_sent((nc - 1) * cs + (cs if ys > 1 else 0) + (1 if cs > 1 else 0))
        if ys > 1:
            passes_sent()
        for i in range(cut):
            resid_sent(i)
        passed_all()

    @pl.when(jnp.logical_not(mid))
    def _():
        cov_wait(nc * ys * cs, send=True)
        pheno_wait(nc * cs, send=True)
        dose_sent(nc * cs)

    def parts_landed(count):
        slot = landed.at[pl.ds(0, count)]
        remote(slot, slot, part_send, part_recv, me).wait_recv()

    @pl.when(in_group)
    def _():
        parts_landed(nc * cs - 1)

    @pl.when(jnp.logical_not(in_group))
    def _():
        parts_landed(nc * cs)

    total = jnp.sum(landed[...], axis=0)
    kind = lax.broadcasted_iota(jnp.int32, total.shape, 0)
    out_ref[...] = jnp.where(kind == 0, total / variants, 10.0 / variants * total)

    def parts_sent(count):
        slot = part.at[pl.ds(0, count)]
        remote(slot, slot, part_send, part_recv, me).wait_send()

    @pl.when(in_group)
    def _():
        parts_sent(owners - 1)

    @pl.when(mid & jnp.logical_not(in_group))
    def _():
        parts_sent(owners)


def local(dosage, covars, phenotypes):
    n = lax.axis_size("tile")
    rows, variants = dosage.shape
    genes = phenotypes.shape[1]
    covs = covars.shape[1]
    samples = rows * n
    cs = 2 if n % 2 == 0 else 1
    ys = 2 if n % (2 * cs) == 0 else 1
    zs = n // (cs * ys)
    lo, hi = zs // 4, zs - zs // 4
    peers = (hi - lo) * cs
    owners = n // ys
    gh = genes // ys
    own = genes // n
    halves = 2
    hw = variants // peers // halves
    blocks = gh // LANES
    cut = -(-blocks // peers)
    dma = pltpu.SemaphoreType.DMA
    out = pl.pallas_call(
        functools.partial(kernel, n, zs, ys, cs, lo, hi, own),
        out_shape=pltpu.VMEM((2, LANES), F32),
        in_specs=[pl.BlockSpec(memory_space=pl.ANY)] * 3,
        out_specs=pl.BlockSpec(memory_space=pltpu.VMEM),
        scratch_shapes=[
            pltpu.VMEM((rows, variants), BF16),
            pltpu.VMEM((rows, covs), F32),
            pltpu.VMEM((rows, gh), F32),
            dma((4 + halves,)), dma((7,)),
            pltpu.VMEM((n, 8, LANES), F32),
            pltpu.VMEM((zs * cs, ys, rows, gh), F32),
            pltpu.VMEM((halves, zs * cs, ys, rows, hw), BF16),
            pltpu.VMEM((halves, samples, hw), BF16),
            pltpu.VMEM((halves, 1, hw), F32),
            pltpu.VMEM((gh + LANES, samples), BF16),
            pltpu.VMEM((2, gh, LANES), F32),
            pltpu.VMEM((owners, 2, LANES), F32),
            pltpu.VMEM((peers, 2, LANES), F32),
            dma((4,)), dma((hi - lo, 3, cut)), dma((halves, zs)), dma((halves,)),
        ],
        compiler_params=pltpu.CompilerParams(collective_id=0, has_side_effects=True),
    )(dosage, covars, phenotypes)
    return out[0, :own], out[1, :own]


def solution(mesh):
    spec = P(("cohort", "tile"), None)
    return jax.shard_map(
        local,
        mesh=mesh,
        in_specs=(spec, spec, spec),
        out_specs=(P(("cohort", "tile")), P(("cohort", "tile"))),
        check_vma=False,
    )
```

```python
import functools

import jax
import jax.numpy as jnp
from jax import lax
from jax.experimental import pallas as pl
from jax.experimental.pallas import tpu as pltpu
from jax.sharding import PartitionSpec as P

LANES = 128
CHUNK = 256
HIGH = lax.Precision.HIGHEST
F32 = jnp.float32
BF16 = jnp.bfloat16


def dot(a, b, ca, cb, precision=None):
    return lax.dot_general(
        a, b, (((ca,), (cb,)), ((), ())), precision=precision, preferred_element_type=F32
    )


def split(a, parts):
    out = []
    for _ in range(parts):
        term = a.astype(BF16)
        out.append(term)
        a = a - term.astype(F32)
    return out


def inverse_factor(gram):
    size = gram.shape[0]
    wide = 2 * size
    row_id = lax.broadcasted_iota(jnp.int32, (size, wide), 0)
    eye = (
        lax.broadcasted_iota(jnp.int32, (size, size), 0)
        == lax.broadcasted_iota(jnp.int32, (size, size), 1)
    ).astype(F32)
    work = jnp.concatenate([gram, eye], axis=1)
    for k in range(0, size, 2):
        one = jnp.broadcast_to(work[:, k : k + 1], (size, wide))
        two = jnp.broadcast_to(work[:, k + 1 : k + 2], (size, wide))
        first = lax.rsqrt(one[k : k + 1, :])
        below = two[k : k + 1, :] * first
        second = lax.rsqrt(two[k + 1 : k + 2, :] - below * below)
        top = work[k : k + 1, :] * first
        low = (work[k + 1 : k + 2, :] - below * top) * second
        left = one * first
        right = (two - left * below) * second
        rest = work - left * top - right * low
        work = jnp.where(
            row_id > k + 1, rest, jnp.where(row_id == k, top, jnp.where(row_id == k + 1, low, work))
        )
    return work[:, size:]


def scan(
    c, y, z, oc, other_row, cs, ys, zs, n, owners, me, place, own, halves, hw, samples, covs,
    blocks, cut, cov_all, raw, dose_all, dres, vscale, pt, acc, part, landed, hand_on, cov_wait, cov_over,
    pheno_wait, pass_residuals, wait_residuals, across_wait, d_recv, remote, send_part,
    in_group, lane_slice,
):
    far = range(2, zs)
    hand_on(0, [1])

    cov_wait(n // cs - 1)
    if cs > 1:
        cov_over(c).start()
    hand_on(0, far)
    hand_on(1, [1])
    if cs > 1:
        cov_over(oc).wait_recv()
    tiles = [
        cov_all[ci, p * ys + yi] for p in range(zs) for ci in range(cs) for yi in range(ys)
    ]
    cov = jnp.concatenate(
        [
            tile[:, i * covs : (i + 1) * covs]
            for tile in tiles
            for i in range(samples // n // 8)
        ],
        axis=0,
    )
    covt = cov.T
    factor = inverse_factor(dot(covt, cov, 1, 0, HIGH))
    basist = dot(factor, covt, 1, 0, HIGH)
    eye = (
        lax.broadcasted_iota(jnp.int32, (covs, covs), 0)
        == lax.broadcasted_iota(jnp.int32, (covs, covs), 1)
    ).astype(F32)
    fix = 1.5 * eye - 0.5 * dot(basist, basist, 1, 1, HIGH)
    basist = dot(fix, basist, 1, 0, HIGH)
    bt_hi, bt_mid, bt_low = [t.astype(F32) for t in split(basist, 3)]
    bt = jnp.concatenate([bt_hi, bt_mid, bt_low], axis=0).astype(BF16)
    b_hi, b_mid, b_low = [t.astype(F32) for t in split(basist.T, 3)]
    basis = jnp.concatenate([b_hi, b_hi, b_hi, b_mid, b_mid, b_low], axis=1).astype(BF16)

    def fitted(coef):
        one, two, three = [t.astype(F32) for t in split(coef, 3)]
        stack = jnp.concatenate([one, two, three, one, two, one], axis=0).astype(BF16)
        return dot(basis, stack, 1, 0)

    def dose_residual(h, j):
        cols = lane_slice(j * CHUNK, CHUNK)
        dose = dose_all[h, :, :, :, cols].reshape(samples, CHUNK)
        coef = dot(bt, dose, 1, 0)
        coef = coef[0:covs] + (coef[covs : 2 * covs] + coef[2 * covs :])
        resid = dose.astype(F32) - fitted(coef)
        dres[h, :, cols] = resid.astype(BF16)
        sumsq = jnp.sum(resid * resid, axis=0, keepdims=True)
        vscale[h, :, cols] = 1.0 / (sumsq + 0.1 * samples)

    def dose_residuals(h):
        if cs > 1:
            slot = dose_all.at[h, other_row, y]
            remote(slot, slot, d_recv.at[h, z], d_recv.at[h, z], me).wait_recv()
        if ys > 1:
            across_wait(h)
        for j in range(hw // CHUNK):
            dose_residual(h, j)

    def residual(b, to):
        at = b * LANES
        pheno = raw[:, :, :, lane_slice(at, LANES)].reshape(samples, LANES)
        hi, mid, low = split(pheno, 3)
        with_hi = dot(bt, hi, 1, 0)
        with_mid = dot(bt[0 : 2 * covs], mid, 1, 0)
        coef = (
            with_hi[0:covs]
            + (with_hi[covs : 2 * covs] + with_mid[0:covs])
            + (with_hi[2 * covs :] + with_mid[covs:] + dot(bt[0:covs], low, 1, 0))
        )
        resid = pheno - fitted(coef)
        var = jnp.sum(resid * resid, axis=0, keepdims=True) / samples + 0.1
        pt[lane_slice(to * LANES, LANES), :] = (resid * lax.rsqrt(var)).astype(BF16).T

    def residuals():
        step = max(g for g in range(1, 8) if cut % g == 0)

        @pl.loop(0, cut // step)
        def _(i):
            for g in range(step):
                b = c * cut + i * step + g
                residual(jnp.minimum(b, blocks - 1), jnp.minimum(b, blocks))

        pass_residuals()

    step = max(g for g in range(1, 8) if blocks % g == 0)

    def associate(h):
        wide = min(2 * CHUNK, hw)

        @pl.loop(0, hw // wide)
        def _(j):
            cols = lane_slice(j * wide, wide)
            scale = vscale[h, :, cols]

            @pl.loop(0, blocks // step)
            def _(i):
                for g in range(step):
                    at = lane_slice((i * step + g) * LANES, LANES)
                    cross = dot(pt[at, :], dres[h, :, cols], 1, 0)
                    chi = cross * cross * scale
                    hit = 1.0 + jnp.tanh(chi - 4.0)
                    acc[0, at, :] += sum(chi[:, i : i + LANES] for i in range(0, wide, LANES))
                    acc[1, at, :] += sum(hit[:, i : i + LANES] for i in range(0, wide, LANES))

    acc[...] = jnp.zeros_like(acc)
    hand_on(1, far)
    dose_residuals(0)
    pheno_wait()
    residuals()
    dose_residuals(1)
    wait_residuals()
    associate(0)
    associate(1)

    line = lax.broadcasted_iota(jnp.int32, (8, 4 * LANES), 0)
    lane = lax.broadcasted_iota(jnp.int32, (8, 4 * LANES), 1)
    pick = (lane // (2 * LANES) == line).astype(F32).astype(BF16)

    @pl.loop(0, owners // 8)
    def _(b):
        for i in range(8):
            j = b * 8 + i
            at = pl.ds(pl.multiple_of(j * own, 8), own)
            terms = split(acc[0, at, :], 2) + split(acc[1, at, :], 2)
            sums = dot(pick, jnp.concatenate(terms, axis=1), 1, 1)
            part[j, :, pl.ds(0, own)] = sums[0:2, :]
        for i in range(8):
            j = b * 8 + i

            @pl.when(y * owners + j != me)
            def _():
                send_part(j)

    @pl.when(in_group)
    def _():
        landed[place] = part[lax.rem(me, owners)]


def kernel(
    n, zs, ys, cs, lo, hi, own,
    dose_in, cov_in, pheno_in, out_ref,
    dose_ref, cov_ref, pheno_ref, load_sem, sends, cov_all, raw, dose_all, dres, vscale, pt, acc,
    part, landed, recvs, heard, d_recv, p_recv,
):
    me = lax.axis_index("tile")
    rows, variants = dose_in.shape
    covs = cov_in.shape[1]
    samples = rows * n
    gh = raw.shape[-1]
    halves = dose_all.shape[0]
    hw = dose_all.shape[-1]
    width = halves * hw
    nc = hi - lo
    owners = n // ys
    c = lax.rem(me, cs)
    y = lax.rem(me // cs, ys)
    z = me // (cs * ys)
    oc = lax.rem(c + 1, cs)
    oy = lax.rem(y + 1, ys)
    place = (z - lo) * cs + c
    own_row = z * cs + c
    other_row = z * cs + oc
    cov_send, b_send, a_send, over_send, d_send, pass_send, part_send, x_send, k_send = [
        sends.at[i] for i in range(9)
    ]
    cov_recv, b_recv, a_recv, part_recv, x_recv, k_recv = [
        recvs.at[i] for i in range(6)
    ]
    mid = (z >= lo) & (z < hi)
    far = (2 * z) // zs

    def index(zi, yi, ci):
        return (zi * ys + yi) * cs + ci

    def remote(src, dst, ssem, rsem, dev):
        return pltpu.make_async_remote_copy(
            src_ref=src, dst_ref=dst, send_sem=ssem, recv_sem=rsem,
            device_id={"tile": dev}, device_id_type=pl.DeviceIdType.MESH,
        )

    def lane_slice(start, size):
        return pl.ds(pl.multiple_of(start, LANES), size)

    loads = [
        pltpu.make_async_copy(cov_in, cov_ref, load_sem.at[0]),
        pltpu.make_async_copy(
            pheno_in.at[:, lane_slice(oy * gh, gh)], pheno_ref, load_sem.at[2]
        ),
        pltpu.make_async_copy(
            pheno_in.at[:, lane_slice(y * gh, gh)], raw.at[own_row, y], load_sem.at[1]
        ),
        pltpu.make_async_copy(dose_in, dose_ref, load_sem.at[3]),
    ]

    def own_dose(h):
        return pltpu.make_async_copy(
            dose_in.at[:, lane_slice(place * width + h * hw, hw)],
            dose_all.at[h, own_row, y], load_sem.at[4 + h],
        )

    for load in loads:
        load.start()

    @pl.when(mid)
    def _():
        for h in range(halves):
            own_dose(h).start()

    barrier = pltpu.get_barrier_semaphore()

    def tell(sem, dev):
        pl.semaphore_signal(
            sem, inc=1, device_id={"tile": dev}, device_id_type=pl.DeviceIdType.MESH
        )

    def tell_plane(sem):
        for dy in range(ys):
            for dc in range(cs):
                if dy or dc:
                    tell(sem, index(z, lax.rem(y + dy, ys), lax.rem(c + dc, cs)))

    tell_plane(barrier)

    @pl.when(z > 0)
    def _():
        tell(barrier, index(z - 1, y, c))

    @pl.when(z + 1 < zs)
    def _():
        tell(barrier, index(z + 1, y, c))

    for load in loads:
        load.wait()
    packed = [cov_ref[g : g + 8, :] for g in range(0, rows, 8)]
    fill = jnp.zeros((8, LANES - len(packed) * covs), F32)
    cov_all[c, z * ys + y] = jnp.concatenate(packed + [fill], axis=1)

    @pl.when(mid)
    def _():
        for h in range(halves):
            own_dose(h).wait()

    if zs > 1:
        @pl.when((z > 0) & (z + 1 < zs))
        def _():
            pl.semaphore_wait(barrier, ys * cs + 1)

        @pl.when((z == 0) | (z + 1 == zs))
        def _():
            pl.semaphore_wait(barrier, ys * cs)
    elif ys * cs > 1:
        pl.semaphore_wait(barrier, ys * cs - 1)
    tell_plane(heard.at[0])

    def hear_plane():
        if ys * cs > 1:
            pl.semaphore_wait(heard.at[0], ys * cs - 1)

    def hear_all():
        @pl.when(z + 1 < hi - 1)
        def _():
            pl.semaphore_wait(heard.at[1], 1)

        @pl.when(z - 1 > lo)
        def _():
            pl.semaphore_wait(heard.at[2], 1)

        @pl.when((z < hi - 1) & (z > 0))
        def _():
            tell(heard.at[1], index(z - 1, y, c))

        @pl.when((z > lo) & (z + 1 < zs))
        def _():
            tell(heard.at[2], index(z + 1, y, c))

    def plane(i, body):
        p = jnp.where(mid, lo + lax.rem(z - lo + 1 + i + nc, nc), lo + i + far * (nc - 1 - 2 * i))

        @pl.when(p != z)
        def _():
            body(p)

    def planes(body):
        for i in range(nc):
            plane(i, body)

    def cov_copies():
        own_cov = cov_all.at[c, z * ys + y]
        for j in range(nc * ys):
            dev = (lo * ys + j) * cs + c

            @pl.when(dev != me)
            def _():
                remote(own_cov, own_cov, cov_send, cov_recv, dev).start()

    def cov_wait(count, send=False):
        slot = cov_all.at[0, pl.ds(0, count)]
        copy = remote(slot, slot, cov_send, cov_recv, me)
        if send:
            copy.wait_send()
        else:
            copy.wait_recv()

    def cov_over(ci):
        slot = cov_all.at[ci]
        return remote(slot, slot, k_send, k_recv, index(z, y, oc))

    def across():
        return remote(pheno_ref, raw.at[own_row, y], b_send, b_recv, index(z, oy, c))

    blocks = gh // LANES
    cut = -(-blocks // cs)

    def genes_of(ci):
        start = min(ci * cut, blocks)
        return pl.ds(start * LANES, min(cut, blocks - start) * LANES)

    def by_core(body):
        for ci in range(cs):
            @pl.when(c == ci)
            def _():
                body(ci)

    def pheno_to(d):
        def to(p):
            for ci in range(cs):
                slot = raw.at[own_row, lax.rem(y + d, ys), :, genes_of(ci)]
                remote(slot, slot, a_send, a_recv, index(p, y, ci)).start()

        return to

    def pheno_over(d):
        def body(ci):
            slot = raw.at[own_row, lax.rem(y + d, ys), :, genes_of((ci + 1) % cs)]
            remote(slot, slot, over_send, a_recv, index(z, y, oc)).start()

        if cs > 1:
            @pl.when(mid)
            def _():
                by_core(body)

    def pheno_wait():
        def body(ci):
            slot = raw.at[pl.ds(0, zs * cs - 1), :, :, genes_of(ci)]
            remote(slot, slot, a_send, a_recv, me).wait_recv()

        by_core(body)

    def pheno_sent(count):
        slot = raw.at[pl.ds(0, count)]
        remote(slot, slot, a_send, a_recv, me).wait_send()

    def over_sent():
        def body(ci):
            slot = raw.at[0, :, :, genes_of((ci + 1) % cs)]
            remote(slot, slot, over_send, a_recv, me).wait_send()

        by_core(body)

    def resid_copy(ci):
        slot = pt.at[genes_of(ci)]
        return remote(slot, slot, x_send, x_recv, index(z, y, oc))

    def pass_residuals():
        if cs > 1:
            by_core(lambda ci: resid_copy(ci).start())

    def wait_residuals():
        if cs > 1:
            by_core(lambda ci: resid_copy((ci + 1) % cs).wait_recv())

    def block(p, ci, h):
        return dose_ref.at[:, lane_slice(((p - lo) * cs + ci) * width + h * hw, hw)]

    def dose_to(h, cores=(0, 1)):
        def to(p):
            for dc in cores[:cs]:
                ci = lax.rem(c + dc, cs)
                remote(
                    block(p, ci, h), dose_all.at[h, own_row, y], d_send, d_recv.at[h, z],
                    index(p, y, ci),
                ).start()

        return to

    def own_copies(h):
        @pl.when(mid)
        def _():
            if ys > 1:
                for ci in range(cs):
                    remote(
                        block(z, ci, h), dose_all.at[h, own_row, y], d_send, p_recv.at[h],
                        index(z, oy, ci),
                    ).start()
            if cs > 1:
                remote(
                    block(z, oc, h), dose_all.at[h, own_row, y], d_send, d_recv.at[h, z],
                    index(z, y, oc),
                ).start()

    def dose_sent(count):
        slot = dose_all.at[:, pl.ds(0, count), 0]
        remote(slot, slot, d_send, d_recv.at[0, 0], me).wait_send()

    def dose_pass(h, p):
        slot = dose_all.at[h, pl.ds(p * cs, cs), y]
        return remote(slot, slot, pass_send, p_recv.at[h], index(z, oy, c))

    def passes_sent():
        slot = dose_all.at[:, pl.ds(0, (zs - 1) * cs), 0]
        remote(slot, slot, pass_send, p_recv.at[0], me).wait_send()

    def dose_wait(h, p):
        slot = dose_all.at[h, pl.ds(p * cs, cs), y]
        return remote(slot, slot, pass_send, d_recv.at[h, p], me)

    def across_wait(h):
        slot = dose_all.at[h, :, oy]
        remote(slot, slot, pass_send, p_recv.at[h], me).wait_recv()

    def at_distance(k, body):
        @pl.when(z >= k)
        def _():
            body(z - k)

        @pl.when(z + k < zs)
        def _():
            body(z + k)

    def hand_on(h, ks):
        def body(p):
            dose_wait(h, p).wait_recv()
            if ys > 1:
                dose_pass(h, p).start()

        for k in ks:
            at_distance(k, body)

    next_door = nc == 2 and lo == 1
    if not next_door:
        hear_plane()
        hear_all()
    if ys > 1:
        across().start()
    own_copies(0)
    plane(0, dose_to(0, (0,)))
    own_copies(1)
    plane(0, dose_to(1, (0,)))
    if next_door:
        hear_plane()
        hear_all()
    if cs > 1:
        plane(0, dose_to(0, (1,)))
    for i in range(1, nc):
        plane(i, dose_to(0))
    cov_copies()
    if cs > 1:
        plane(0, dose_to(1, (1,)))
    for i in range(1, nc):
        plane(i, dose_to(1))
    pheno_over(0)
    for i in range(nc):
        plane(i, pheno_to(0))
    if ys > 1:
        slot = raw.at[own_row, oy]
        remote(slot, slot, b_send, b_recv, me).wait_recv()
        pheno_over(1)
        for i in range(nc):
            plane(i, pheno_to(1))

    in_group = mid & (me // owners == y)

    def send_part(j):
        remote(part.at[j], landed.at[place], part_send, part_recv, y * owners + j).start()

    @pl.when(mid)
    def _():
        scan(
            c, y, z, oc, other_row, cs, ys, zs, n, owners, me, place, own, halves, hw, samples,
            covs, blocks, cut, cov_all, raw, dose_all, dres, vscale, pt, acc, part, landed,
            hand_on, cov_wait, cov_over, pheno_wait, pass_residuals, wait_residuals, across_wait, d_recv,
            remote, send_part, in_group, lane_slice,
        )

    if ys > 1:
        across().wait_send()

    @pl.when(mid)
    def _():
        cov_wait(nc * ys - 1, send=True)
        if cs > 1:
            cov_over(c).wait_send()
        if nc > 1:
            pheno_sent(nc - 1)
        if cs > 1:
            over_sent()
            by_core(lambda ci: resid_copy(ci).wait_send())
        dose_sent((nc - 1) * cs + (cs if ys > 1 else 0) + (1 if cs > 1 else 0))
        if ys > 1:
            passes_sent()

    @pl.when(jnp.logical_not(mid))
    def _():
        cov_wait(nc * ys, send=True)
        pheno_sent(nc)
        dose_sent(nc * cs)

    def parts_landed(count):
        slot = landed.at[pl.ds(0, count)]
        remote(slot, slot, part_send, part_recv, me).wait_recv()

    @pl.when(in_group)
    def _():
        parts_landed(nc * cs - 1)

    @pl.when(jnp.logical_not(in_group))
    def _():
        parts_landed(nc * cs)

    total = jnp.sum(landed[...], axis=0)
    kind = lax.broadcasted_iota(jnp.int32, total.shape, 0)
    out_ref[...] = jnp.where(kind == 0, total / variants, 10.0 / variants * total)

    def parts_sent(count):
        slot = part.at[pl.ds(0, count)]
        remote(slot, slot, part_send, part_recv, me).wait_send()

    @pl.when(in_group)
    def _():
        parts_sent(owners - 1)

    @pl.when(mid & jnp.logical_not(in_group))
    def _():
        parts_sent(owners)


def local(dosage, covars, phenotypes):
    n = lax.axis_size("tile")
    rows, variants = dosage.shape
    genes = phenotypes.shape[1]
    covs = covars.shape[1]
    samples = rows * n
    cs = 2 if n % 2 == 0 else 1
    ys = 2 if n % (2 * cs) == 0 else 1
    zs = n // (cs * ys)
    lo, hi = zs // 4, zs - zs // 4
    peers = (hi - lo) * cs
    owners = n // ys
    gh = genes // ys
    own = genes // n
    halves = 2
    hw = variants // peers // halves
    blocks = gh // LANES
    dma = pltpu.SemaphoreType.DMA
    out = pl.pallas_call(
        functools.partial(kernel, n, zs, ys, cs, lo, hi, own),
        out_shape=pltpu.VMEM((2, LANES), F32),
        in_specs=[pl.BlockSpec(memory_space=pl.ANY)] * 3,
        out_specs=pl.BlockSpec(memory_space=pltpu.VMEM),
        scratch_shapes=[
            pltpu.VMEM((rows, variants), BF16),
            pltpu.VMEM((rows, covs), F32),
            pltpu.VMEM((rows, gh), F32),
            dma((4 + halves,)), dma((9,)),
            pltpu.VMEM((cs, n // cs, 8, LANES), F32),
            pltpu.VMEM((zs * cs, ys, rows, gh), F32),
            pltpu.VMEM((halves, zs * cs, ys, rows, hw), BF16),
            pltpu.VMEM((halves, samples, hw), BF16),
            pltpu.VMEM((halves, 1, hw), F32),
            pltpu.VMEM((gh + LANES, samples), BF16),
            pltpu.VMEM((2, gh, LANES), F32),
            pltpu.VMEM((owners, 2, LANES), F32),
            pltpu.VMEM((peers, 2, LANES), F32),
            dma((6,)), pltpu.SemaphoreType.REGULAR((3,)), dma((halves, zs)), dma((halves,)),
        ],
        compiler_params=pltpu.CompilerParams(collective_id=0, has_side_effects=True),
    )(dosage, covars, phenotypes)
    return out[0, :own], out[1, :own]


def solution(mesh):
    spec = P(("cohort", "tile"), None)
    return jax.shard_map(
        local,
        mesh=mesh,
        in_specs=(spec, spec, spec),
        out_specs=(P(("cohort", "tile")), P(("cohort", "tile"))),
        check_vma=False,
    )
```

```python
import functools

import jax
import jax.numpy as jnp
from jax import lax
from jax.experimental import pallas as pl
from jax.experimental.pallas import tpu as pltpu
from jax.sharding import PartitionSpec as P

LANES = 128
CHUNK = 256
HIGH = lax.Precision.HIGHEST
F32 = jnp.float32
BF16 = jnp.bfloat16


def dot(a, b, ca, cb, precision=None):
    return lax.dot_general(
        a, b, (((ca,), (cb,)), ((), ())), precision=precision, preferred_element_type=F32
    )


def split(a, parts):
    out = []
    for _ in range(parts):
        term = a.astype(BF16)
        out.append(term)
        a = a - term.astype(F32)
    return out


def inverse_factor(gram):
    size = gram.shape[0]
    wide = 2 * size
    row_id = lax.broadcasted_iota(jnp.int32, (size, wide), 0)
    eye = (
        lax.broadcasted_iota(jnp.int32, (size, size), 0)
        == lax.broadcasted_iota(jnp.int32, (size, size), 1)
    ).astype(F32)
    work = jnp.concatenate([gram, eye], axis=1)
    for k in range(0, size, 2):
        one = jnp.broadcast_to(work[:, k : k + 1], (size, wide))
        two = jnp.broadcast_to(work[:, k + 1 : k + 2], (size, wide))
        first = lax.rsqrt(one[k : k + 1, :])
        below = two[k : k + 1, :] * first
        second = lax.rsqrt(two[k + 1 : k + 2, :] - below * below)
        top = work[k : k + 1, :] * first
        low = (work[k + 1 : k + 2, :] - below * top) * second
        left = one * first
        right = (two - left * below) * second
        rest = work - left * top - right * low
        work = jnp.where(
            row_id > k + 1, rest, jnp.where(row_id == k, top, jnp.where(row_id == k + 1, low, work))
        )
    return work[:, size:]


def scan(
    c, y, z, oc, other_row, cs, ys, zs, n, owners, me, place, own, halves, hw, samples, covs,
    blocks, cut, cov_all, raw, dose_all, dres, vscale, pt, acc, part, landed, hand_on, cov_wait, cov_over,
    pheno_wait, pass_residuals, wait_residuals, across_wait, d_recv, remote, send_part,
    in_group, lane_slice,
):
    far = range(2, zs)
    hand_on(0, [1])

    cov_wait(n // cs - 1)
    if cs > 1:
        cov_over(c).start()
    hand_on(0, far)
    hand_on(1, [1])
    if cs > 1:
        cov_over(oc).wait_recv()
    tiles = [
        cov_all[ci, p * ys + yi] for p in range(zs) for ci in range(cs) for yi in range(ys)
    ]
    cov = jnp.concatenate(
        [
            tile[:, i * covs : (i + 1) * covs]
            for tile in tiles
            for i in range(samples // n // 8)
        ],
        axis=0,
    )
    covt = cov.T
    factor = inverse_factor(dot(covt, cov, 1, 0, HIGH))
    basist = dot(factor, covt, 1, 0, HIGH)
    eye = (
        lax.broadcasted_iota(jnp.int32, (covs, covs), 0)
        == lax.broadcasted_iota(jnp.int32, (covs, covs), 1)
    ).astype(F32)
    fix = 1.5 * eye - 0.5 * dot(basist, basist, 1, 1, HIGH)
    basist = dot(fix, basist, 1, 0, HIGH)
    bt_hi, bt_mid, bt_low = [t.astype(F32) for t in split(basist, 3)]
    bt = jnp.concatenate([bt_hi, bt_mid, bt_low], axis=0).astype(BF16)
    b_hi, b_mid, b_low = [t.astype(F32) for t in split(basist.T, 3)]
    basis = jnp.concatenate([b_hi, b_hi, b_hi, b_mid, b_mid, b_low], axis=1).astype(BF16)

    def fitted(coef):
        one, two, three = [t.astype(F32) for t in split(coef, 3)]
        stack = jnp.concatenate([one, two, three, one, two, one], axis=0).astype(BF16)
        return dot(basis, stack, 1, 0)

    def dose_residual(h, j):
        cols = lane_slice(j * CHUNK, CHUNK)
        dose = dose_all[h, :, :, :, cols].reshape(samples, CHUNK)
        coef = dot(bt, dose, 1, 0)
        coef = coef[0:covs] + (coef[covs : 2 * covs] + coef[2 * covs :])
        resid = dose.astype(F32) - fitted(coef)
        dres[h, :, cols] = resid.astype(BF16)
        sumsq = jnp.sum(resid * resid, axis=0, keepdims=True)
        vscale[h, :, cols] = 1.0 / (sumsq + 0.1 * samples)

    def dose_residuals(h):
        if cs > 1:
            slot = dose_all.at[h, other_row, y]
            remote(slot, slot, d_recv.at[h, z], d_recv.at[h, z], me).wait_recv()
        if ys > 1:
            across_wait(h)
        for j in range(hw // CHUNK):
            dose_residual(h, j)

    def residual(b, to):
        at = b * LANES
        pheno = raw[:, :, :, lane_slice(at, LANES)].reshape(samples, LANES)
        hi, mid, low = split(pheno, 3)
        with_hi = dot(bt, hi, 1, 0)
        with_mid = dot(bt[0 : 2 * covs], mid, 1, 0)
        coef = (
            with_hi[0:covs]
            + (with_hi[covs : 2 * covs] + with_mid[0:covs])
            + (with_hi[2 * covs :] + with_mid[covs:] + dot(bt[0:covs], low, 1, 0))
        )
        resid = pheno - fitted(coef)
        var = jnp.sum(resid * resid, axis=0, keepdims=True) / samples + 0.1
        pt[lane_slice(to * LANES, LANES), :] = (resid * lax.rsqrt(var)).astype(BF16).T

    def residuals():
        step = max(g for g in range(1, 8) if cut % g == 0)

        @pl.loop(0, cut // step)
        def _(i):
            for g in range(step):
                b = c * cut + i * step + g
                residual(jnp.minimum(b, blocks - 1), jnp.minimum(b, blocks))

        pass_residuals()

    def associate(h, start, stop):
        wide = hw
        count = stop - start
        step = max(g for g in range(1, 8) if count % g == 0)

        @pl.loop(0, hw // wide)
        def _(j):
            cols = lane_slice(j * wide, wide)
            scale = vscale[h, :, cols]

            @pl.loop(0, count // step)
            def _(i):
                for g in range(step):
                    at = lane_slice((start + i * step + g) * LANES, LANES)
                    cross = dot(pt[at, :], dres[h, :, cols], 1, 0)
                    chi = cross * cross * scale
                    hit = 1.0 + jnp.tanh(chi - 4.0)
                    acc[0, at, :] += sum(chi[:, i : i + LANES] for i in range(0, wide, LANES))
                    acc[1, at, :] += sum(hit[:, i : i + LANES] for i in range(0, wide, LANES))

    line = lax.broadcasted_iota(jnp.int32, (8, 4 * LANES), 0)
    lane = lax.broadcasted_iota(jnp.int32, (8, 4 * LANES), 1)
    pick = (lane // (2 * LANES) == line).astype(F32).astype(BF16)

    def parts(start, stop):
        for j in range(start, stop):
            at = pl.ds(j * own, own)
            terms = split(acc[0, at, :], 2) + split(acc[1, at, :], 2)
            sums = dot(pick, jnp.concatenate(terms, axis=1), 1, 1)
            part[j, :, pl.ds(0, own)] = sums[0:2, :]
        for j in range(start, stop):
            @pl.when(y * owners + j != me)
            def _():
                send_part(j)

    acc[...] = jnp.zeros_like(acc)
    hand_on(1, far)
    dose_residuals(0)
    pheno_wait()
    residuals()
    dose_residuals(1)
    wait_residuals()
    at = owner = 0
    for stop in (-(-blocks * 2 // 7), -(-blocks * 4 // 7), blocks):
        for h in range(halves):
            associate(h, at, stop)
        ready = stop * LANES // own if stop < blocks else owners
        parts(owner, ready)
        at, owner = stop, ready

    @pl.when(in_group)
    def _():
        landed[place] = part[lax.rem(me, owners)]


def kernel(
    n, zs, ys, cs, lo, hi, own,
    dose_in, cov_in, pheno_in, out_ref,
    dose_ref, cov_ref, pheno_ref, load_sem, sends, cov_all, raw, dose_all, dres, vscale, pt, acc,
    part, landed, recvs, heard, d_recv, p_recv,
):
    me = lax.axis_index("tile")
    rows, variants = dose_in.shape
    covs = cov_in.shape[1]
    samples = rows * n
    gh = raw.shape[-1]
    halves = dose_all.shape[0]
    hw = dose_all.shape[-1]
    width = halves * hw
    nc = hi - lo
    owners = n // ys
    c = lax.rem(me, cs)
    y = lax.rem(me // cs, ys)
    z = me // (cs * ys)
    oc = lax.rem(c + 1, cs)
    oy = lax.rem(y + 1, ys)
    place = (z - lo) * cs + c
    own_row = z * cs + c
    other_row = z * cs + oc
    cov_send, b_send, a_send, over_send, d_send, pass_send, part_send, x_send, k_send = [
        sends.at[i] for i in range(9)
    ]
    cov_recv, b_recv, a_recv, part_recv, x_recv, k_recv = [
        recvs.at[i] for i in range(6)
    ]
    mid = (z >= lo) & (z < hi)
    far = (2 * z) // zs

    def index(zi, yi, ci):
        return (zi * ys + yi) * cs + ci

    def remote(src, dst, ssem, rsem, dev):
        return pltpu.make_async_remote_copy(
            src_ref=src, dst_ref=dst, send_sem=ssem, recv_sem=rsem,
            device_id={"tile": dev}, device_id_type=pl.DeviceIdType.MESH,
        )

    def lane_slice(start, size):
        return pl.ds(pl.multiple_of(start, LANES), size)

    loads = [
        pltpu.make_async_copy(cov_in, cov_ref, load_sem.at[0]),
        pltpu.make_async_copy(
            pheno_in.at[:, lane_slice(oy * gh, gh)], pheno_ref, load_sem.at[2]
        ),
        pltpu.make_async_copy(
            pheno_in.at[:, lane_slice(y * gh, gh)], raw.at[own_row, y], load_sem.at[1]
        ),
        pltpu.make_async_copy(dose_in, dose_ref, load_sem.at[3]),
    ]

    def own_dose(h):
        return pltpu.make_async_copy(
            dose_in.at[:, lane_slice(place * width + h * hw, hw)],
            dose_all.at[h, own_row, y], load_sem.at[4 + h],
        )

    for load in loads:
        load.start()

    @pl.when(mid)
    def _():
        for h in range(halves):
            own_dose(h).start()

    barrier = pltpu.get_barrier_semaphore()

    def tell(sem, dev):
        pl.semaphore_signal(
            sem, inc=1, device_id={"tile": dev}, device_id_type=pl.DeviceIdType.MESH
        )

    def tell_plane(sem):
        for dy in range(ys):
            for dc in range(cs):
                if dy or dc:
                    tell(sem, index(z, lax.rem(y + dy, ys), lax.rem(c + dc, cs)))

    tell_plane(barrier)

    @pl.when(z > 0)
    def _():
        tell(barrier, index(z - 1, y, c))

    @pl.when(z + 1 < zs)
    def _():
        tell(barrier, index(z + 1, y, c))

    for load in loads:
        load.wait()
    packed = [cov_ref[g : g + 8, :] for g in range(0, rows, 8)]
    fill = jnp.zeros((8, LANES - len(packed) * covs), F32)
    cov_all[c, z * ys + y] = jnp.concatenate(packed + [fill], axis=1)

    @pl.when(mid)
    def _():
        for h in range(halves):
            own_dose(h).wait()

    if zs > 1:
        @pl.when((z > 0) & (z + 1 < zs))
        def _():
            pl.semaphore_wait(barrier, ys * cs + 1)

        @pl.when((z == 0) | (z + 1 == zs))
        def _():
            pl.semaphore_wait(barrier, ys * cs)
    elif ys * cs > 1:
        pl.semaphore_wait(barrier, ys * cs - 1)
    tell_plane(heard.at[0])

    def hear_plane():
        if ys * cs > 1:
            pl.semaphore_wait(heard.at[0], ys * cs - 1)

    def hear_all():
        @pl.when(z + 1 < hi - 1)
        def _():
            pl.semaphore_wait(heard.at[1], 1)

        @pl.when(z - 1 > lo)
        def _():
            pl.semaphore_wait(heard.at[2], 1)

        @pl.when((z < hi - 1) & (z > 0))
        def _():
            tell(heard.at[1], index(z - 1, y, c))

        @pl.when((z > lo) & (z + 1 < zs))
        def _():
            tell(heard.at[2], index(z + 1, y, c))

    def plane(i, body):
        p = jnp.where(mid, lo + lax.rem(z - lo + 1 + i + nc, nc), lo + i + far * (nc - 1 - 2 * i))

        @pl.when(p != z)
        def _():
            body(p)

    def planes(body):
        for i in range(nc):
            plane(i, body)

    def cov_copies():
        own_cov = cov_all.at[c, z * ys + y]
        for j in range(nc * ys):
            dev = (lo * ys + j) * cs + c

            @pl.when(dev != me)
            def _():
                remote(own_cov, own_cov, cov_send, cov_recv, dev).start()

    def cov_wait(count, send=False):
        slot = cov_all.at[0, pl.ds(0, count)]
        copy = remote(slot, slot, cov_send, cov_recv, me)
        if send:
            copy.wait_send()
        else:
            copy.wait_recv()

    def cov_over(ci):
        slot = cov_all.at[ci]
        return remote(slot, slot, k_send, k_recv, index(z, y, oc))

    def across():
        return remote(pheno_ref, raw.at[own_row, y], b_send, b_recv, index(z, oy, c))

    blocks = gh // LANES
    cut = -(-blocks // cs)

    def genes_of(ci):
        start = min(ci * cut, blocks)
        return pl.ds(start * LANES, min(cut, blocks - start) * LANES)

    def by_core(body):
        for ci in range(cs):
            @pl.when(c == ci)
            def _():
                body(ci)

    def pheno_to(d):
        def to(p):
            for ci in range(cs):
                slot = raw.at[own_row, lax.rem(y + d, ys), :, genes_of(ci)]
                remote(slot, slot, a_send, a_recv, index(p, y, ci)).start()

        return to

    def pheno_over(d):
        def body(ci):
            slot = raw.at[own_row, lax.rem(y + d, ys), :, genes_of((ci + 1) % cs)]
            remote(slot, slot, over_send, a_recv, index(z, y, oc)).start()

        if cs > 1:
            @pl.when(mid)
            def _():
                by_core(body)

    def pheno_wait():
        def body(ci):
            slot = raw.at[pl.ds(0, zs * cs - 1), :, :, genes_of(ci)]
            remote(slot, slot, a_send, a_recv, me).wait_recv()

        by_core(body)

    def pheno_sent(count):
        slot = raw.at[pl.ds(0, count)]
        remote(slot, slot, a_send, a_recv, me).wait_send()

    def over_sent():
        def body(ci):
            slot = raw.at[0, :, :, genes_of((ci + 1) % cs)]
            remote(slot, slot, over_send, a_recv, me).wait_send()

        by_core(body)

    def resid_copy(ci):
        slot = pt.at[genes_of(ci)]
        return remote(slot, slot, x_send, x_recv, index(z, y, oc))

    def pass_residuals():
        if cs > 1:
            by_core(lambda ci: resid_copy(ci).start())

    def wait_residuals():
        if cs > 1:
            by_core(lambda ci: resid_copy((ci + 1) % cs).wait_recv())

    def block(p, ci, h):
        return dose_ref.at[:, lane_slice(((p - lo) * cs + ci) * width + h * hw, hw)]

    def dose_to(h, cores=(0, 1)):
        def to(p):
            for dc in cores[:cs]:
                ci = lax.rem(c + dc, cs)
                remote(
                    block(p, ci, h), dose_all.at[h, own_row, y], d_send, d_recv.at[h, z],
                    index(p, y, ci),
                ).start()

        return to

    def own_copies(h):
        @pl.when(mid)
        def _():
            if ys > 1:
                for ci in range(cs):
                    remote(
                        block(z, ci, h), dose_all.at[h, own_row, y], d_send, p_recv.at[h],
                        index(z, oy, ci),
                    ).start()
            if cs > 1:
                remote(
                    block(z, oc, h), dose_all.at[h, own_row, y], d_send, d_recv.at[h, z],
                    index(z, y, oc),
                ).start()

    def dose_sent(count):
        slot = dose_all.at[:, pl.ds(0, count), 0]
        remote(slot, slot, d_send, d_recv.at[0, 0], me).wait_send()

    def dose_pass(h, p):
        slot = dose_all.at[h, pl.ds(p * cs, cs), y]
        return remote(slot, slot, pass_send, p_recv.at[h], index(z, oy, c))

    def passes_sent():
        slot = dose_all.at[:, pl.ds(0, (zs - 1) * cs), 0]
        remote(slot, slot, pass_send, p_recv.at[0], me).wait_send()

    def dose_wait(h, p):
        slot = dose_all.at[h, pl.ds(p * cs, cs), y]
        return remote(slot, slot, pass_send, d_recv.at[h, p], me)

    def across_wait(h):
        slot = dose_all.at[h, :, oy]
        remote(slot, slot, pass_send, p_recv.at[h], me).wait_recv()

    def at_distance(k, body):
        @pl.when(z >= k)
        def _():
            body(z - k)

        @pl.when(z + k < zs)
        def _():
            body(z + k)

    def hand_on(h, ks):
        def body(p):
            dose_wait(h, p).wait_recv()
            if ys > 1:
                dose_pass(h, p).start()

        for k in ks:
            at_distance(k, body)

    next_door = nc == 2 and lo == 1
    if not next_door:
        hear_plane()
        hear_all()
    if ys > 1:
        across().start()
    own_copies(0)
    plane(0, dose_to(0, (0,)))
    own_copies(1)
    plane(0, dose_to(1, (0,)))
    if next_door:
        hear_plane()
        hear_all()
    if cs > 1:
        plane(0, dose_to(0, (1,)))
    for i in range(1, nc):
        plane(i, dose_to(0))
    cov_copies()
    if cs > 1:
        plane(0, dose_to(1, (1,)))
    for i in range(1, nc):
        plane(i, dose_to(1))
    pheno_over(0)
    for i in range(nc):
        plane(i, pheno_to(0))
    if ys > 1:
        slot = raw.at[own_row, oy]
        remote(slot, slot, b_send, b_recv, me).wait_recv()
        pheno_over(1)
        for i in range(nc):
            plane(i, pheno_to(1))

    in_group = mid & (me // owners == y)

    def send_part(j):
        remote(part.at[j], landed.at[place], part_send, part_recv, y * owners + j).start()

    @pl.when(mid)
    def _():
        scan(
            c, y, z, oc, other_row, cs, ys, zs, n, owners, me, place, own, halves, hw, samples,
            covs, blocks, cut, cov_all, raw, dose_all, dres, vscale, pt, acc, part, landed,
            hand_on, cov_wait, cov_over, pheno_wait, pass_residuals, wait_residuals, across_wait, d_recv,
            remote, send_part, in_group, lane_slice,
        )

    if ys > 1:
        across().wait_send()

    @pl.when(mid)
    def _():
        cov_wait(nc * ys - 1, send=True)
        if cs > 1:
            cov_over(c).wait_send()
        if nc > 1:
            pheno_sent(nc - 1)
        if cs > 1:
            over_sent()
            by_core(lambda ci: resid_copy(ci).wait_send())
        dose_sent((nc - 1) * cs + (cs if ys > 1 else 0) + (1 if cs > 1 else 0))
        if ys > 1:
            passes_sent()

    @pl.when(jnp.logical_not(mid))
    def _():
        cov_wait(nc * ys, send=True)
        pheno_sent(nc)
        dose_sent(nc * cs)

    def parts_landed(count):
        slot = landed.at[pl.ds(0, count)]
        remote(slot, slot, part_send, part_recv, me).wait_recv()

    @pl.when(in_group)
    def _():
        parts_landed(nc * cs - 1)

    @pl.when(jnp.logical_not(in_group))
    def _():
        parts_landed(nc * cs)

    total = jnp.sum(landed[...], axis=0)
    kind = lax.broadcasted_iota(jnp.int32, total.shape, 0)
    out_ref[...] = jnp.where(kind == 0, total / variants, 10.0 / variants * total)

    def parts_sent(count):
        slot = part.at[pl.ds(0, count)]
        remote(slot, slot, part_send, part_recv, me).wait_send()

    @pl.when(in_group)
    def _():
        parts_sent(owners - 1)

    @pl.when(mid & jnp.logical_not(in_group))
    def _():
        parts_sent(owners)


def local(dosage, covars, phenotypes):
    n = lax.axis_size("tile")
    rows, variants = dosage.shape
    genes = phenotypes.shape[1]
    covs = covars.shape[1]
    samples = rows * n
    cs = 2 if n % 2 == 0 else 1
    ys = 2 if n % (2 * cs) == 0 else 1
    zs = n // (cs * ys)
    lo, hi = zs // 4, zs - zs // 4
    peers = (hi - lo) * cs
    owners = n // ys
    gh = genes // ys
    own = genes // n
    halves = 2
    hw = variants // peers // halves
    blocks = gh // LANES
    dma = pltpu.SemaphoreType.DMA
    out = pl.pallas_call(
        functools.partial(kernel, n, zs, ys, cs, lo, hi, own),
        out_shape=pltpu.VMEM((2, LANES), F32),
        in_specs=[pl.BlockSpec(memory_space=pl.ANY)] * 3,
        out_specs=pl.BlockSpec(memory_space=pltpu.VMEM),
        scratch_shapes=[
            pltpu.VMEM((rows, variants), BF16),
            pltpu.VMEM((rows, covs), F32),
            pltpu.VMEM((rows, gh), F32),
            dma((4 + halves,)), dma((9,)),
            pltpu.VMEM((cs, n // cs, 8, LANES), F32),
            pltpu.VMEM((zs * cs, ys, rows, gh), F32),
            pltpu.VMEM((halves, zs * cs, ys, rows, hw), BF16),
            pltpu.VMEM((halves, samples, hw), BF16),
            pltpu.VMEM((halves, 1, hw), F32),
            pltpu.VMEM((gh + LANES, samples), BF16),
            pltpu.VMEM((2, gh, LANES), F32),
            pltpu.VMEM((owners, 2, LANES), F32),
            pltpu.VMEM((peers, 2, LANES), F32),
            dma((6,)), pltpu.SemaphoreType.REGULAR((3,)), dma((halves, zs)), dma((halves,)),
        ],
        compiler_params=pltpu.CompilerParams(collective_id=0, has_side_effects=True),
    )(dosage, covars, phenotypes)
    return out[0, :own], out[1, :own]


def solution(mesh):
    spec = P(("cohort", "tile"), None)
    return jax.shard_map(
        local,
        mesh=mesh,
        in_specs=(spec, spec, spec),
        out_specs=(P(("cohort", "tile")), P(("cohort", "tile"))),
        check_vma=False,
    )
```

```python
import functools

import jax
import jax.numpy as jnp
from jax import lax
from jax.experimental import pallas as pl
from jax.experimental.pallas import tpu as pltpu
from jax.sharding import PartitionSpec as P

LANES = 128
CHUNK = 256
HIGH = lax.Precision.HIGHEST
F32 = jnp.float32
BF16 = jnp.bfloat16


def dot(a, b, ca, cb, precision=None):
    return lax.dot_general(
        a, b, (((ca,), (cb,)), ((), ())), precision=precision, preferred_element_type=F32
    )


def split(a, parts):
    out = []
    for _ in range(parts):
        term = a.astype(BF16)
        out.append(term)
        a = a - term.astype(F32)
    return out


def inverse_factor(gram):
    size = gram.shape[0]
    wide = 2 * size
    row_id = lax.broadcasted_iota(jnp.int32, (size, wide), 0)
    eye = (
        lax.broadcasted_iota(jnp.int32, (size, size), 0)
        == lax.broadcasted_iota(jnp.int32, (size, size), 1)
    ).astype(F32)
    work = jnp.concatenate([gram, eye], axis=1)
    for k in range(0, size, 2):
        one = jnp.broadcast_to(work[:, k : k + 1], (size, wide))
        two = jnp.broadcast_to(work[:, k + 1 : k + 2], (size, wide))
        first = lax.rsqrt(one[k : k + 1, :])
        below = two[k : k + 1, :] * first
        second = lax.rsqrt(two[k + 1 : k + 2, :] - below * below)
        top = work[k : k + 1, :] * first
        low = (work[k + 1 : k + 2, :] - below * top) * second
        left = one * first
        right = (two - left * below) * second
        rest = work - left * top - right * low
        work = jnp.where(
            row_id > k + 1, rest, jnp.where(row_id == k, top, jnp.where(row_id == k + 1, low, work))
        )
    return work[:, size:]


def scan(
    c, y, z, oc, other_row, cs, ys, zs, n, owners, me, place, own, halves, hw, samples, covs,
    blocks, cut, cov_all, raw, dose_all, dres, vscale, pt, acc, part, landed, hand_on, cov_wait, cov_over,
    pheno_wait, pass_residuals, wait_residuals, across_wait, d_recv, remote, send_part,
    in_group, lane_slice,
):
    far = range(2, zs)
    hand_on(0, [1])

    cov_wait(n // cs - 1)
    if cs > 1:
        cov_over(c).start()
    hand_on(0, far)
    hand_on(1, [1])
    if cs > 1:
        cov_over(oc).wait_recv()
    tiles = [
        cov_all[ci, p * ys + yi] for p in range(zs) for ci in range(cs) for yi in range(ys)
    ]
    cov = jnp.concatenate(
        [
            tile[:, i * covs : (i + 1) * covs]
            for tile in tiles
            for i in range(samples // n // 8)
        ],
        axis=0,
    )
    covt = cov.T
    factor = inverse_factor(dot(covt, cov, 1, 0, HIGH))
    basist = dot(factor, covt, 1, 0, HIGH)
    eye = (
        lax.broadcasted_iota(jnp.int32, (covs, covs), 0)
        == lax.broadcasted_iota(jnp.int32, (covs, covs), 1)
    ).astype(F32)
    fix = 1.5 * eye - 0.5 * dot(basist, basist, 1, 1, HIGH)
    basist = dot(fix, basist, 1, 0, HIGH)
    bt_hi, bt_mid, bt_low = [t.astype(F32) for t in split(basist, 3)]
    bt = jnp.concatenate([bt_hi, bt_mid, bt_low], axis=0).astype(BF16)
    b_hi, b_mid, b_low = [t.astype(F32) for t in split(basist.T, 3)]
    basis = jnp.concatenate([b_hi, b_hi, b_hi, b_mid, b_mid, b_low], axis=1).astype(BF16)

    def fitted(coef):
        one, two, three = [t.astype(F32) for t in split(coef, 3)]
        stack = jnp.concatenate([one, two, three, one, two, one], axis=0).astype(BF16)
        return dot(basis, stack, 1, 0)

    def dose_residual(h, j):
        cols = lane_slice(j * CHUNK, CHUNK)
        dose = dose_all[h, :, :, :, cols].reshape(samples, CHUNK)
        coef = dot(bt, dose, 1, 0)
        coef = coef[0:covs] + (coef[covs : 2 * covs] + coef[2 * covs :])
        resid = dose.astype(F32) - fitted(coef)
        dres[h, :, cols] = resid.astype(BF16)
        sumsq = jnp.sum(resid * resid, axis=0, keepdims=True)
        vscale[h, :, cols] = 1.0 / (sumsq + 0.1 * samples)

    def dose_residuals(h):
        if cs > 1:
            slot = dose_all.at[h, other_row, y]
            remote(slot, slot, d_recv.at[h, z], d_recv.at[h, z], me).wait_recv()
        if ys > 1:
            across_wait(h)
        for j in range(hw // CHUNK):
            dose_residual(h, j)

    wide = max(g for g in range(1, 5) if cut % g == 0)

    def residual(b):
        genes = raw[:, :, :, lane_slice(b * LANES, wide * LANES)]
        pheno = genes.reshape(samples, wide * LANES)
        hi, mid, low = split(pheno, 3)
        with_hi = dot(bt, hi, 1, 0)
        with_mid = dot(bt[0 : 2 * covs], mid, 1, 0)
        coef = (
            with_hi[0:covs]
            + (with_hi[covs : 2 * covs] + with_mid[0:covs])
            + (with_hi[2 * covs :] + with_mid[covs:] + dot(bt[0:covs], low, 1, 0))
        )
        resid = pheno - fitted(coef)
        var = jnp.sum(resid * resid, axis=0, keepdims=True) / samples + 0.1
        resid = (resid * lax.rsqrt(var)).astype(BF16).T
        for g in range(wide):
            to = jnp.where((b + g) // cut == c, b + g, blocks)
            pt[lane_slice(to * LANES, LANES), :] = resid[g * LANES : (g + 1) * LANES]

    def residuals():
        @pl.loop(0, cut // wide)
        def _(i):
            residual(jnp.minimum(c * cut + i * wide, blocks - wide))

        pass_residuals()

    def associate(start, stop):
        count = stop - start
        step = max(g for g in range(1, 5) if count % g == 0)

        def group(first):
            for g in range(step):
                at = lane_slice((first + g) * LANES, LANES)
                chis, hits = [], []
                for h in range(halves):
                    cross = dot(pt[at, :], dres[h], 1, 0)
                    chi = cross * cross * vscale[h]
                    hit = 1.0 + jnp.tanh(chi - 4.0)
                    chis += [chi[:, i : i + LANES] for i in range(0, hw, LANES)]
                    hits += [hit[:, i : i + LANES] for i in range(0, hw, LANES)]
                acc[0, at, :] = sum(chis)
                acc[1, at, :] = sum(hits)

        if count == step:
            group(start)
        else:
            @pl.loop(0, count // step)
            def _(i):
                group(start + i * step)

    line = lax.broadcasted_iota(jnp.int32, (8, 4 * LANES), 0)
    lane = lax.broadcasted_iota(jnp.int32, (8, 4 * LANES), 1)
    pick = (lane // (2 * LANES) == line).astype(F32).astype(BF16)

    def parts(start, stop):
        for j in range(start, stop):
            at = pl.ds(j * own, own)
            terms = split(acc[0, at, :], 2) + split(acc[1, at, :], 2)
            sums = dot(pick, jnp.concatenate(terms, axis=1), 1, 1)
            part[j, :, pl.ds(0, own)] = sums[0:2, :]
        for j in range(start, stop):
            @pl.when(y * owners + j != me)
            def _():
                send_part(j)

    hand_on(1, far)
    dose_residuals(0)
    pheno_wait()
    residuals()
    dose_residuals(1)
    wait_residuals()
    at = owner = 0
    for stop in (-(-blocks * 2 // 7), -(-blocks * 4 // 7), blocks):
        associate(at, stop)
        ready = stop * LANES // own if stop < blocks else owners
        parts(owner, ready)
        at, owner = stop, ready

    @pl.when(in_group)
    def _():
        landed[place] = part[lax.rem(me, owners)]


def kernel(
    n, zs, ys, cs, lo, hi, own,
    dose_in, cov_in, pheno_in, out_ref,
    dose_ref, cov_ref, pheno_ref, load_sem, sends, cov_all, raw, dose_all, dres, vscale, pt, acc,
    part, landed, recvs, heard, d_recv, p_recv,
):
    me = lax.axis_index("tile")
    rows, variants = dose_in.shape
    covs = cov_in.shape[1]
    samples = rows * n
    gh = raw.shape[-1]
    halves = dose_all.shape[0]
    hw = dose_all.shape[-1]
    width = halves * hw
    nc = hi - lo
    owners = n // ys
    c = lax.rem(me, cs)
    y = lax.rem(me // cs, ys)
    z = me // (cs * ys)
    oc = lax.rem(c + 1, cs)
    oy = lax.rem(y + 1, ys)
    place = (z - lo) * cs + c
    own_row = z * cs + c
    other_row = z * cs + oc
    cov_send, b_send, a_send, over_send, d_send, pass_send, part_send, x_send, k_send = [
        sends.at[i] for i in range(9)
    ]
    cov_recv, b_recv, a_recv, part_recv, x_recv, k_recv = [
        recvs.at[i] for i in range(6)
    ]
    mid = (z >= lo) & (z < hi)
    far = (2 * z) // zs

    def index(zi, yi, ci):
        return (zi * ys + yi) * cs + ci

    def remote(src, dst, ssem, rsem, dev):
        return pltpu.make_async_remote_copy(
            src_ref=src, dst_ref=dst, send_sem=ssem, recv_sem=rsem,
            device_id={"tile": dev}, device_id_type=pl.DeviceIdType.MESH,
        )

    def lane_slice(start, size):
        return pl.ds(pl.multiple_of(start, LANES), size)

    loads = [
        pltpu.make_async_copy(cov_in, cov_ref, load_sem.at[0]),
        pltpu.make_async_copy(
            pheno_in.at[:, lane_slice(oy * gh, gh)], pheno_ref, load_sem.at[2]
        ),
        pltpu.make_async_copy(
            pheno_in.at[:, lane_slice(y * gh, gh)], raw.at[own_row, y], load_sem.at[1]
        ),
        pltpu.make_async_copy(dose_in, dose_ref, load_sem.at[3]),
    ]

    def own_dose(h):
        return pltpu.make_async_copy(
            dose_in.at[:, lane_slice(place * width + h * hw, hw)],
            dose_all.at[h, own_row, y], load_sem.at[4 + h],
        )

    for load in loads:
        load.start()

    @pl.when(mid)
    def _():
        for h in range(halves):
            own_dose(h).start()

    barrier = pltpu.get_barrier_semaphore()

    def tell(sem, dev):
        pl.semaphore_signal(
            sem, inc=1, device_id={"tile": dev}, device_id_type=pl.DeviceIdType.MESH
        )

    def tell_plane(sem):
        for dy in range(ys):
            for dc in range(cs):
                if dy or dc:
                    tell(sem, index(z, lax.rem(y + dy, ys), lax.rem(c + dc, cs)))

    tell_plane(barrier)

    @pl.when(z > 0)
    def _():
        for ci in range(cs):
            tell(barrier, index(z - 1, y, ci))

    @pl.when(z + 1 < zs)
    def _():
        for ci in range(cs):
            tell(barrier, index(z + 1, y, ci))

    for load in loads:
        load.wait()
    packed = [cov_ref[g : g + 8, :] for g in range(0, rows, 8)]
    fill = jnp.zeros((8, LANES - len(packed) * covs), F32)
    cov_all[c, z * ys + y] = jnp.concatenate(packed + [fill], axis=1)

    @pl.when(mid)
    def _():
        for h in range(halves):
            own_dose(h).wait()

    if zs > 1:
        @pl.when((z > 0) & (z + 1 < zs))
        def _():
            pl.semaphore_wait(barrier, ys * cs - 1 + 2 * cs)

        @pl.when((z == 0) | (z + 1 == zs))
        def _():
            pl.semaphore_wait(barrier, ys * cs - 1 + cs)
    elif ys * cs > 1:
        pl.semaphore_wait(barrier, ys * cs - 1)
    tell_plane(heard.at[0])

    def hear_plane():
        if ys * cs > 1:
            pl.semaphore_wait(heard.at[0], ys * cs - 1)

    def hear_all():
        @pl.when(z + 1 < hi - 1)
        def _():
            pl.semaphore_wait(heard.at[1], 1)

        @pl.when(z - 1 > lo)
        def _():
            pl.semaphore_wait(heard.at[2], 1)

        @pl.when((z < hi - 1) & (z > 0))
        def _():
            tell(heard.at[1], index(z - 1, y, c))

        @pl.when((z > lo) & (z + 1 < zs))
        def _():
            tell(heard.at[2], index(z + 1, y, c))

    def plane(i, body):
        p = jnp.where(mid, lo + lax.rem(z - lo + 1 + i + nc, nc), lo + i + far * (nc - 1 - 2 * i))

        @pl.when(p != z)
        def _():
            body(p)

    def planes(body):
        for i in range(nc):
            plane(i, body)

    def cov_copies():
        own_cov = cov_all.at[c, z * ys + y]
        for j in range(nc * ys):
            dev = (lo * ys + j) * cs + c

            @pl.when(dev != me)
            def _():
                remote(own_cov, own_cov, cov_send, cov_recv, dev).start()

    def cov_wait(count, send=False):
        slot = cov_all.at[0, pl.ds(0, count)]
        copy = remote(slot, slot, cov_send, cov_recv, me)
        if send:
            copy.wait_send()
        else:
            copy.wait_recv()

    def cov_over(ci):
        slot = cov_all.at[ci]
        return remote(slot, slot, k_send, k_recv, index(z, y, oc))

    def across():
        return remote(pheno_ref, raw.at[own_row, y], b_send, b_recv, index(z, oy, c))

    blocks = gh // LANES
    cut = -(-blocks // cs)

    def genes_of(ci):
        start = min(ci * cut, blocks)
        return pl.ds(start * LANES, min(cut, blocks - start) * LANES)

    def by_core(body):
        for ci in range(cs):
            @pl.when(c == ci)
            def _():
                body(ci)

    def pheno_to(d):
        def to(p):
            for ci in range(cs):
                slot = raw.at[own_row, lax.rem(y + d, ys), :, genes_of(ci)]
                remote(slot, slot, a_send, a_recv, index(p, y, ci)).start()

        return to

    def pheno_over(d):
        def body(ci):
            slot = raw.at[own_row, lax.rem(y + d, ys), :, genes_of((ci + 1) % cs)]
            remote(slot, slot, over_send, a_recv, index(z, y, oc)).start()

        if cs > 1:
            @pl.when(mid)
            def _():
                by_core(body)

    def pheno_wait():
        def body(ci):
            slot = raw.at[pl.ds(0, zs * cs - 1), :, :, genes_of(ci)]
            remote(slot, slot, a_send, a_recv, me).wait_recv()

        by_core(body)

    def pheno_sent(count):
        slot = raw.at[pl.ds(0, count)]
        remote(slot, slot, a_send, a_recv, me).wait_send()

    def over_sent():
        def body(ci):
            slot = raw.at[0, :, :, genes_of((ci + 1) % cs)]
            remote(slot, slot, over_send, a_recv, me).wait_send()

        by_core(body)

    def resid_copy(ci):
        slot = pt.at[genes_of(ci)]
        return remote(slot, slot, x_send, x_recv, index(z, y, oc))

    def pass_residuals():
        if cs > 1:
            by_core(lambda ci: resid_copy(ci).start())

    def wait_residuals():
        if cs > 1:
            by_core(lambda ci: resid_copy((ci + 1) % cs).wait_recv())

    def block(p, ci, h):
        return dose_ref.at[:, lane_slice(((p - lo) * cs + ci) * width + h * hw, hw)]

    def dose_to(h, cores=(0, 1)):
        def to(p):
            for dc in cores[:cs]:
                ci = lax.rem(c + dc, cs)
                remote(
                    block(p, ci, h), dose_all.at[h, own_row, y], d_send, d_recv.at[h, z],
                    index(p, y, ci),
                ).start()

        return to

    def own_copies(h):
        @pl.when(mid)
        def _():
            if ys > 1:
                for ci in range(cs):
                    remote(
                        block(z, ci, h), dose_all.at[h, own_row, y], d_send, p_recv.at[h],
                        index(z, oy, ci),
                    ).start()
            if cs > 1:
                remote(
                    block(z, oc, h), dose_all.at[h, own_row, y], d_send, d_recv.at[h, z],
                    index(z, y, oc),
                ).start()

    def dose_sent(count):
        slot = dose_all.at[:, pl.ds(0, count), 0]
        remote(slot, slot, d_send, d_recv.at[0, 0], me).wait_send()

    def dose_pass(h, p):
        slot = dose_all.at[h, pl.ds(p * cs, cs), y]
        return remote(slot, slot, pass_send, p_recv.at[h], index(z, oy, c))

    def passes_sent():
        slot = dose_all.at[:, pl.ds(0, (zs - 1) * cs), 0]
        remote(slot, slot, pass_send, p_recv.at[0], me).wait_send()

    def dose_wait(h, p):
        slot = dose_all.at[h, pl.ds(p * cs, cs), y]
        return remote(slot, slot, pass_send, d_recv.at[h, p], me)

    def across_wait(h):
        slot = dose_all.at[h, :, oy]
        remote(slot, slot, pass_send, p_recv.at[h], me).wait_recv()

    def at_distance(k, body):
        @pl.when(z >= k)
        def _():
            body(z - k)

        @pl.when(z + k < zs)
        def _():
            body(z + k)

    def hand_on(h, ks):
        def body(p):
            dose_wait(h, p).wait_recv()
            if ys > 1:
                dose_pass(h, p).start()

        for k in ks:
            at_distance(k, body)

    next_door = nc == 2 and lo == 1
    if not next_door:
        hear_plane()
        hear_all()
    if ys > 1:
        across().start()
    own_copies(0)
    plane(0, dose_to(0))
    own_copies(1)
    pheno_over(0)
    plane(0, pheno_to(0))
    if next_door:
        hear_plane()
        hear_all()
    for i in range(1, nc):
        plane(i, dose_to(0))
    cov_copies()
    plane(0, dose_to(1))
    for i in range(1, nc):
        plane(i, dose_to(1))
    for i in range(1, nc):
        plane(i, pheno_to(0))
    if ys > 1:
        slot = raw.at[own_row, oy]
        remote(slot, slot, b_send, b_recv, me).wait_recv()
        pheno_over(1)
        for i in range(nc):
            plane(i, pheno_to(1))

    in_group = mid & (me // owners == y)

    def send_part(j):
        remote(part.at[j], landed.at[place], part_send, part_recv, y * owners + j).start()

    @pl.when(mid)
    def _():
        scan(
            c, y, z, oc, other_row, cs, ys, zs, n, owners, me, place, own, halves, hw, samples,
            covs, blocks, cut, cov_all, raw, dose_all, dres, vscale, pt, acc, part, landed,
            hand_on, cov_wait, cov_over, pheno_wait, pass_residuals, wait_residuals, across_wait, d_recv,
            remote, send_part, in_group, lane_slice,
        )

    if ys > 1:
        across().wait_send()

    @pl.when(mid)
    def _():
        cov_wait(nc * ys - 1, send=True)
        if cs > 1:
            cov_over(c).wait_send()
        if nc > 1:
            pheno_sent(nc - 1)
        if cs > 1:
            over_sent()
            by_core(lambda ci: resid_copy(ci).wait_send())
        dose_sent((nc - 1) * cs + (cs if ys > 1 else 0) + (1 if cs > 1 else 0))
        if ys > 1:
            passes_sent()

    @pl.when(jnp.logical_not(mid))
    def _():
        cov_wait(nc * ys, send=True)
        pheno_sent(nc)
        dose_sent(nc * cs)

    def parts_landed(count):
        slot = landed.at[pl.ds(0, count)]
        remote(slot, slot, part_send, part_recv, me).wait_recv()

    @pl.when(in_group)
    def _():
        parts_landed(nc * cs - 1)

    @pl.when(jnp.logical_not(in_group))
    def _():
        parts_landed(nc * cs)

    total = jnp.sum(landed[...], axis=0)
    kind = lax.broadcasted_iota(jnp.int32, total.shape, 0)
    out_ref[...] = jnp.where(kind == 0, total / variants, 10.0 / variants * total)

    def parts_sent(count):
        slot = part.at[pl.ds(0, count)]
        remote(slot, slot, part_send, part_recv, me).wait_send()

    @pl.when(in_group)
    def _():
        parts_sent(owners - 1)

    @pl.when(mid & jnp.logical_not(in_group))
    def _():
        parts_sent(owners)


def local(dosage, covars, phenotypes):
    n = lax.axis_size("tile")
    rows, variants = dosage.shape
    genes = phenotypes.shape[1]
    covs = covars.shape[1]
    samples = rows * n
    cs = 2 if n % 2 == 0 else 1
    ys = 2 if n % (2 * cs) == 0 else 1
    zs = n // (cs * ys)
    lo, hi = zs // 4, zs - zs // 4
    peers = (hi - lo) * cs
    owners = n // ys
    gh = genes // ys
    own = genes // n
    halves = 2
    hw = variants // peers // halves
    blocks = gh // LANES
    dma = pltpu.SemaphoreType.DMA
    out = pl.pallas_call(
        functools.partial(kernel, n, zs, ys, cs, lo, hi, own),
        out_shape=pltpu.VMEM((2, LANES), F32),
        in_specs=[pl.BlockSpec(memory_space=pl.ANY)] * 3,
        out_specs=pl.BlockSpec(memory_space=pltpu.VMEM),
        scratch_shapes=[
            pltpu.VMEM((rows, variants), BF16),
            pltpu.VMEM((rows, covs), F32),
            pltpu.VMEM((rows, gh), F32),
            dma((4 + halves,)), dma((9,)),
            pltpu.VMEM((cs, n // cs, 8, LANES), F32),
            pltpu.VMEM((zs * cs, ys, rows, gh), F32),
            pltpu.VMEM((halves, zs * cs, ys, rows, hw), BF16),
            pltpu.VMEM((halves, samples, hw), BF16),
            pltpu.VMEM((halves, 1, hw), F32),
            pltpu.VMEM((gh + LANES, samples), BF16),
            pltpu.VMEM((2, gh, LANES), F32),
            pltpu.VMEM((owners, 2, LANES), F32),
            pltpu.VMEM((peers, 2, LANES), F32),
            dma((6,)), pltpu.SemaphoreType.REGULAR((3,)), dma((halves, zs)), dma((halves,)),
        ],
        compiler_params=pltpu.CompilerParams(collective_id=0, has_side_effects=True),
    )(dosage, covars, phenotypes)
    return out[0, :own], out[1, :own]


def solution(mesh):
    spec = P(("cohort", "tile"), None)
    return jax.shard_map(
        local,
        mesh=mesh,
        in_specs=(spec, spec, spec),
        out_specs=(P(("cohort", "tile")), P(("cohort", "tile"))),
        check_vma=False,
    )
```
